32 devices in a mesh: lat: 16 (over z, x, core), chan: 2 (over y).
Axes of the slice: x: 2, y: 2, z: 4, core: 2. Of those that a mesh axis runs over, the one named last changes fastest.
Arguments:
- spec_in: bfloat16 [384, 1, 256, 2, 384], P('lat', None, 'chan'), may hold values from -6 to 6
- legendre: float32 [384, 384, 384], P('lat'), may hold values from -0.4375 to 0.4375
- mode_slot: int32 [384], replicated, may hold values from 0 to 383, each once
- w_in: bfloat16 [512, 256], replicated, may hold values from -0.375 to 0.375
- b_in: float32 [512], replicated, may hold values from -3 to 3
- w_out: bfloat16 [256, 512], replicated, may hold values from -0.25 to 0.25
- kernel: float32 [256, 9], P('chan'), may hold values from -4 to 4
Outputs:
- spec_out: bfloat16 [384, 1, 256, 2, 384], P('lat', None, 'chan')
The draws below stay inside these ranges and needn't reach their ends.
Inputs may be any that keep to these rules, and one draw needn't show every extreme that they name: mode_slot holds every number of 0 to 383 once.
All inputs are finite; a program needn't handle non-finite values.
Results may differ from the reference program's by a relative error of at most 0.0083.
Values may be sent and summed in bfloat16 or wider, within the bound.
A program may use at most 192 MiB of HBM per device.

```python
import math
import jax
import jax.numpy as jnp
from jax import lax

C = 256
H = 512
NLAT = 384
NLON = 768
M = 384
L = 384
B = 1


def steps_of(rng, shape, pieces, low, high):
    gain, own = 1.0, jax.random.fold_in(rng, 6)
    for axis_at, parts in pieces:
        draws = jnp.exp(jax.random.uniform(jax.random.fold_in(own, axis_at), (parts,), jnp.float32, low / len(pieces), high / len(pieces)))
        gain = gain * jnp.repeat(draws, shape[axis_at] // parts).reshape([-1 if axis == axis_at else 1 for axis in range(len(shape))])
    return gain


def scatter_about(key, extent, deviation, most, pieces=(), kind=jnp.bfloat16):
    drawn = deviation * jax.random.normal(key, extent, jnp.float32)
    if pieces:
        drawn = drawn * steps_of(key, extent, pieces, -0.22, 0.18)
    return jnp.clip(drawn, -most, most).astype(kind)


def setup_inputs(seed: int = 0) -> dict:
    key_list = jax.random.split(jax.random.key(seed), 8)
    spec_in = scatter_about(key_list[0], (M, B, C, 2, L), 1.0, 6.0, ((0, 16), (2, 2)))
    legendre = scatter_about(key_list[1], (M, NLAT, L), (L // 2) ** -0.5, 0.4375, ((0, 16),), jnp.float32)
    mode_slot = jax.random.permutation(key_list[2], M).astype(jnp.int32)
    w_in = scatter_about(key_list[3], (H, C), C ** -0.5, 0.375)
    b_in = scatter_about(key_list[4], (H,), 0.5, 3.0, (), jnp.float32)
    w_out = scatter_about(key_list[5], (C, H), H ** -0.5, 0.25)
    kernel = scatter_about(key_list[6], (C, 9), 0.3, 4.0, ((0, 2),), jnp.float32)
    return {"spec_in": spec_in, "legendre": legendre, "mode_slot": mode_slot, "w_in": w_in, "b_in": b_in, "w_out": w_out, "kernel": kernel}


def wave_table(modes, count):
    columns = jnp.arange(count, dtype=jnp.int32)
    phase = (modes[:, None] * columns[None, :]) % count
    angle = phase.astype(jnp.float32) * (2.0 * math.pi / count)
    factor = count ** -0.5
    return jnp.stack([jnp.cos(angle) * factor, -jnp.sin(angle) * factor], axis=1)


def reference(spec_in, legendre, mode_slot, w_in, b_in, w_out, kernel):
    high = lax.Precision.HIGHEST
    degrees = jnp.arange(L, dtype=jnp.int32)
    masked = jnp.where(degrees[None, None, :] >= mode_slot[:, None, None], legendre, jnp.float32(0.0))
    waves = wave_table(mode_slot, NLON)
    half = NLON // 2

    def one_sample(coeffs):
        coeff = jnp.einsum('scrl,stl->scrt', coeffs.astype(jnp.float32), masked, precision=high)
        grid = jnp.einsum('scrt,srp->tcp', coeff, waves, precision=high).astype(jnp.bfloat16)
        pre = jnp.einsum('kc,tcp->tkp', w_in.astype(jnp.float32), grid.astype(jnp.float32), precision=high)
        hidden = jax.nn.gelu(pre + b_in[None, :, None], approximate=True).astype(jnp.bfloat16)
        branch = jnp.einsum('ck,tkp->tcp', w_out.astype(jnp.float32), hidden.astype(jnp.float32), precision=high)
        mixed = (grid.astype(jnp.float32) + branch).astype(jnp.bfloat16)
        wide = mixed.astype(jnp.float32)
        rows = jnp.concatenate([jnp.roll(wide[0:1], half, axis=2), wide, jnp.roll(wide[-1:], half, axis=2)], axis=0)
        conv = jnp.zeros_like(wide)
        for i in range(3):
            band = rows[i:i + NLAT]
            for j in range(3):
                conv = conv + kernel[:, 3 * i + j][None, :, None] * jnp.roll(band, 1 - j, axis=2)
        field = wide + conv
        modes = jnp.einsum('tcp,srp->scrt', field, waves, precision=high)
        return jnp.einsum('scrt,stl->scrl', modes, masked, precision=high).astype(jnp.bfloat16)

    result = lax.map(one_sample, jnp.moveaxis(spec_in, 1, 0))
    return jnp.moveaxis(result, 0, 1)
```

```python
import functools
import math

import jax
import jax.numpy as jnp
from jax import lax
from jax.experimental import pallas as pl
from jax.experimental.pallas import tpu as pltpu
from jax.sharding import PartitionSpec as P

NLON = 768


def with_halo(array, sides, width):
    for axis, dim in sides:
        count, length = (lax.axis_size(axis), array.shape[dim])
        up = [(i, (i + 1) % count) for i in range(count - 1)]
        down = [(j, i) for i, j in up]
        last = lax.slice_in_dim(array, length - width, length, axis=dim)
        first = lax.slice_in_dim(array, 0, width, axis=dim)
        before = lax.ppermute(last, axis, up)
        after = lax.ppermute(first, axis, down)
        array = jnp.concatenate([before, array, after], axis=dim)
    return array


def wave_table(modes, count):
    columns = jnp.arange(count, dtype=jnp.int32)
    phase = modes[:, None] * columns[None, :] % count
    angle = phase.astype(jnp.float32) * (2.0 * math.pi / count)
    factor = count ** (-0.5)
    return jnp.stack([jnp.cos(angle) * factor, -jnp.sin(angle) * factor], axis=1)


def on_device(spec_in, legendre, mode_slot, w_in, b_in, w_out, kernel):
    high = lax.Precision.HIGHEST
    slots_here = legendre.shape[0]
    lat_index = lax.axis_index("lat")
    local_modes = lax.dynamic_slice_in_dim(mode_slot, lat_index * slots_here, slots_here)
    degrees = jnp.arange(legendre.shape[2], dtype=jnp.int32)
    masked = jnp.where(
        degrees[None, None, :] >= local_modes[:, None, None], legendre, jnp.float32(0.0)
    )
    waves = wave_table(mode_slot, NLON)
    coeff = jnp.einsum("sbcrl,stl->sbcrt", spec_in.astype(jnp.float32), masked, precision=high)
    grid = jnp.einsum(
        "sbcrt,srp->btcp",
        lax.all_to_all(coeff, "lat", split_axis=4, concat_axis=0, tiled=True),
        waves,
        precision=high,
    ).astype(jnp.bfloat16)
    batch, rows_here, chan_here, columns = grid.shape
    whole = lax.all_gather(grid, "chan", axis=2, tiled=True)
    chan_index = lax.axis_index("chan")
    w_local = lax.dynamic_slice_in_dim(w_out, chan_index * chan_here, chan_here, 0)
    pre = jnp.einsum("hc,btcp->bthp", w_in, whole, preferred_element_type=jnp.float32)
    hidden = jax.nn.gelu(pre + b_in[None, None, :, None], approximate=True).astype(jnp.bfloat16)
    branch = jnp.einsum("ch,bthp->btcp", w_local, hidden, preferred_element_type=jnp.float32)
    mixed = (grid.astype(jnp.float32) + branch).astype(jnp.bfloat16)
    half = columns // 2
    last_row = lax.axis_size("lat") - 1
    padded = with_halo(mixed, (("lat", 1),), 1)
    upper = jnp.where(lat_index == 0, jnp.roll(mixed[:, 0:1], half, axis=3), padded[:, 0:1])
    lower = jnp.where(lat_index == last_row, jnp.roll(mixed[:, -1:], half, axis=3), padded[:, -1:])
    stacked = jnp.concatenate([upper, padded[:, 1:-1], lower], axis=1).astype(jnp.float32)
    wide = mixed.astype(jnp.float32)
    conv = jnp.zeros_like(wide)
    for i in range(3):
        band = stacked[:, i : i + rows_here]
        for j in range(3):
            conv = conv + kernel[:, 3 * i + j][None, None, :, None] * jnp.roll(band, 1 - j, axis=3)
    field = wide + conv
    modes = jnp.einsum("btcp,srp->sbcrt", field, waves, precision=high)
    return jnp.einsum(
        "sbcrt,stl->sbcrl",
        lax.all_to_all(modes, "lat", split_axis=0, concat_axis=4, tiled=True),
        masked,
        precision=high,
    ).astype(jnp.bfloat16)


def rows_kernel(lats, chans, coeff_ref, waves_t_ref, waves_ref, w_in_ref, b_in_ref, w_out_ref, modes_ref,
                recv, send, fwd_sent, fwd_got, bwd_sent, bwd_got):
    chunks, count, rows, depth, width = coeff_ref.shape
    lat, chan = lax.axis_index("lat"), lax.axis_index("chan")
    me = lat * chans + chan

    def landing(k):
        return recv.at[k, :, chan, pl.ds(lat * depth, depth), :]

    def leaving(k, to):
        return send.at[k, :, to % chans, pl.ds((to // chans) * depth, depth), :]

    def forward(k, _):
        def to_peer(i, _):
            to = (me + i) % count
            pltpu.make_async_remote_copy(
                src_ref=coeff_ref.at[k, to], dst_ref=landing(k),
                send_sem=fwd_sent, recv_sem=fwd_got.at[k],
                device_id=(to // chans, to % chans), device_id_type=pl.DeviceIdType.MESH,
            ).start()
            return 0

        pltpu.make_async_copy(coeff_ref.at[k, me], landing(k), fwd_got.at[k]).start()
        return lax.fori_loop(1, count, to_peer, 0)

    lax.fori_loop(0, chunks, forward, 0)

    def one_chunk(k, _):
        pltpu.make_async_copy(recv.at[k], recv.at[k], fwd_got.at[k]).wait()

        def one_row(j, _):
            merged = jnp.concatenate([recv[k, j, i] for i in range(chans)], axis=1)
            grid = jnp.dot(waves_t_ref[...], merged, preferred_element_type=jnp.float32).astype(jnp.bfloat16)
            pre = jnp.dot(grid, w_in_ref[...], preferred_element_type=jnp.float32) + b_in_ref[...]
            hidden = jax.nn.gelu(pre, approximate=True).astype(jnp.bfloat16)
            branch = jnp.dot(hidden, w_out_ref[...], preferred_element_type=jnp.float32)
            mixed = (grid.astype(jnp.float32) + branch).astype(jnp.bfloat16)
            modes = jnp.dot(waves_ref[...], mixed, preferred_element_type=jnp.float32).astype(jnp.bfloat16)
            for i in range(chans):
                send[k, j, i] = modes[:, i * width : (i + 1) * width]
            return 0

        lax.fori_loop(0, rows, one_row, 0)

        def to_peer(i, _):
            to = (me + i) % count
            pltpu.make_async_remote_copy(
                src_ref=leaving(k, to), dst_ref=modes_ref.at[k, me],
                send_sem=bwd_sent, recv_sem=bwd_got,
                device_id=(to // chans, to % chans), device_id_type=pl.DeviceIdType.MESH,
            ).start()
            return 0

        pltpu.make_async_copy(leaving(k, me), modes_ref.at[k, me], bwd_got).start()
        return lax.fori_loop(1, count, to_peer, 0)

    lax.fori_loop(0, chunks, one_chunk, 0)
    away = coeff_ref.at[:, pl.ds(0, count - 1)]
    pltpu.make_async_copy(away, away, fwd_sent).wait()
    away = modes_ref.at[:, pl.ds(0, count - 1)]
    pltpu.make_async_copy(away, away, bwd_sent).wait()
    pltpu.make_async_copy(modes_ref, modes_ref, bwd_got).wait()


def spectral_filters(kernel, modes, count):
    angle = modes.astype(jnp.float32) * (2.0 * math.pi / count)
    cosine, sine = jnp.cos(angle)[:, None], jnp.sin(angle)[:, None]
    pairs = []
    for i in range(3):
        left, here, right = (kernel[:, 3 * i + j][None, :] for j in range(3))
        pairs.append((here + (left + right) * cosine + (1.0 if i == 1 else 0.0), (right - left) * sine))
    return pairs


def on_device_rows(spec_in, legendre, mode_slot, w_in, b_in, w_out, kernel):
    lats, chans = lax.axis_size("lat"), lax.axis_size("chan")
    count = lats * chans
    slots, rows_all, degrees_all = legendre.shape
    width = spec_in.shape[2]
    own_rows = rows_all // count
    chunks = next(k for k in (4, 3, 2, 1) if own_rows % k == 0)
    rows = own_rows // chunks
    columns = NLON
    lat_index = lax.axis_index("lat")
    local_modes = lax.dynamic_slice_in_dim(mode_slot, lat_index * slots, slots)
    degrees = jnp.arange(degrees_all, dtype=jnp.int32)
    keep = degrees[None, None, :] >= local_modes[:, None, None]
    masked = jnp.where(keep, legendre, jnp.float32(0.0)).astype(jnp.bfloat16)
    waves = wave_table(mode_slot, columns).astype(jnp.bfloat16)
    waves = jnp.swapaxes(waves.reshape(lats, slots, 2, columns), 1, 2).reshape(-1, columns)
    coeff = jnp.einsum("scrl,stl->trsc", spec_in[:, 0], masked, preferred_element_type=jnp.float32)
    coeff = coeff.astype(jnp.bfloat16).reshape(chunks, count, rows, 2 * slots, width)
    hbm, vmem = pl.BlockSpec(memory_space=pl.ANY), pl.BlockSpec(memory_space=pltpu.VMEM)
    modes = pl.pallas_call(
        functools.partial(rows_kernel, lats, chans),
        out_shape=jax.ShapeDtypeStruct(coeff.shape, jnp.bfloat16),
        in_specs=[hbm] + [vmem] * 5,
        out_specs=hbm,
        scratch_shapes=[
            pltpu.VMEM((chunks, rows, chans, lats * 2 * slots, width), jnp.bfloat16),
            pltpu.VMEM((chunks, rows, chans, lats * 2 * slots, width), jnp.bfloat16),
            pltpu.SemaphoreType.DMA,
            pltpu.SemaphoreType.DMA((chunks,)),
            pltpu.SemaphoreType.DMA,
            pltpu.SemaphoreType.DMA,
        ],
        compiler_params=pltpu.CompilerParams(vmem_limit_bytes=48 * 1024 * 1024, has_side_effects=True),
        name="rows",
    )(coeff, waves.T, waves, w_in.T, b_in[None, :], w_out.T)
    modes = modes.reshape(rows_all, 2, slots, width).astype(jnp.float32)
    sign = jnp.where(local_modes % 2 == 0, 1.0, -1.0)[None, None, :, None]
    above = jnp.concatenate([modes[:1] * sign, modes[:-1]], axis=0)
    below = jnp.concatenate([modes[1:], modes[-1:] * sign], axis=0)
    real = imag = 0.0
    for (a, b), x in zip(spectral_filters(kernel, local_modes, columns), (above, modes, below)):
        real = real + a * x[:, 0] - b * x[:, 1]
        imag = imag + a * x[:, 1] + b * x[:, 0]
    field = jnp.stack([real, imag], axis=1).astype(jnp.bfloat16)
    out = jnp.einsum("trsc,stl->scrl", field, masked, preferred_element_type=jnp.float32)
    return out.astype(jnp.bfloat16)[:, None]


def solution(mesh):
    in_specs = (
        P("lat", None, "chan", None, None),
        P("lat", None, None),
        P(),
        P(),
        P(),
        P(),
        P("chan", None),
    )
    out_specs = P("lat", None, "chan", None, None)
    count = mesh.shape["lat"] * mesh.shape["chan"]

    def call(spec_in, legendre, *rest):
        samples, rows_all = spec_in.shape[1], legendre.shape[1]
        by_rows = samples == 1 and rows_all % count == 0
        body = on_device_rows if by_rows else on_device
        return jax.shard_map(
            body, mesh=mesh, in_specs=in_specs, out_specs=out_specs, check_vma=False
        )(spec_in, legendre, *rest)

    return call
```

```python
import functools
import math

import jax
import jax.numpy as jnp
from jax import lax
from jax.experimental import pallas as pl
from jax.experimental.pallas import tpu as pltpu
from jax.sharding import PartitionSpec as P

NLON = 768


def with_halo(array, sides, width):
    for axis, dim in sides:
        count, length = (lax.axis_size(axis), array.shape[dim])
        up = [(i, (i + 1) % count) for i in range(count - 1)]
        down = [(j, i) for i, j in up]
        last = lax.slice_in_dim(array, length - width, length, axis=dim)
        first = lax.slice_in_dim(array, 0, width, axis=dim)
        before = lax.ppermute(last, axis, up)
        after = lax.ppermute(first, axis, down)
        array = jnp.concatenate([before, array, after], axis=dim)
    return array


def wave_table(modes, count):
    columns = jnp.arange(count, dtype=jnp.int32)
    phase = modes[:, None] * columns[None, :] % count
    angle = phase.astype(jnp.float32) * (2.0 * math.pi / count)
    factor = count ** (-0.5)
    return jnp.stack([jnp.cos(angle) * factor, -jnp.sin(angle) * factor], axis=1)


def on_device(spec_in, legendre, mode_slot, w_in, b_in, w_out, kernel):
    high = lax.Precision.HIGHEST
    slots_here = legendre.shape[0]
    lat_index = lax.axis_index("lat")
    local_modes = lax.dynamic_slice_in_dim(mode_slot, lat_index * slots_here, slots_here)
    degrees = jnp.arange(legendre.shape[2], dtype=jnp.int32)
    masked = jnp.where(
        degrees[None, None, :] >= local_modes[:, None, None], legendre, jnp.float32(0.0)
    )
    waves = wave_table(mode_slot, NLON)
    coeff = jnp.einsum("sbcrl,stl->sbcrt", spec_in.astype(jnp.float32), masked, precision=high)
    grid = jnp.einsum(
        "sbcrt,srp->btcp",
        lax.all_to_all(coeff, "lat", split_axis=4, concat_axis=0, tiled=True),
        waves,
        precision=high,
    ).astype(jnp.bfloat16)
    batch, rows_here, chan_here, columns = grid.shape
    whole = lax.all_gather(grid, "chan", axis=2, tiled=True)
    chan_index = lax.axis_index("chan")
    w_local = lax.dynamic_slice_in_dim(w_out, chan_index * chan_here, chan_here, 0)
    pre = jnp.einsum("hc,btcp->bthp", w_in, whole, preferred_element_type=jnp.float32)
    hidden = jax.nn.gelu(pre + b_in[None, None, :, None], approximate=True).astype(jnp.bfloat16)
    branch = jnp.einsum("ch,bthp->btcp", w_local, hidden, preferred_element_type=jnp.float32)
    mixed = (grid.astype(jnp.float32) + branch).astype(jnp.bfloat16)
    half = columns // 2
    last_row = lax.axis_size("lat") - 1
    padded = with_halo(mixed, (("lat", 1),), 1)
    upper = jnp.where(lat_index == 0, jnp.roll(mixed[:, 0:1], half, axis=3), padded[:, 0:1])
    lower = jnp.where(lat_index == last_row, jnp.roll(mixed[:, -1:], half, axis=3), padded[:, -1:])
    stacked = jnp.concatenate([upper, padded[:, 1:-1], lower], axis=1).astype(jnp.float32)
    wide = mixed.astype(jnp.float32)
    conv = jnp.zeros_like(wide)
    for i in range(3):
        band = stacked[:, i : i + rows_here]
        for j in range(3):
            conv = conv + kernel[:, 3 * i + j][None, None, :, None] * jnp.roll(band, 1 - j, axis=3)
    field = wide + conv
    modes = jnp.einsum("btcp,srp->sbcrt", field, waves, precision=high)
    return jnp.einsum(
        "sbcrt,stl->sbcrl",
        lax.all_to_all(modes, "lat", split_axis=0, concat_axis=4, tiled=True),
        masked,
        precision=high,
    ).astype(jnp.bfloat16)


GROUP = 8
LANES = 128


def cosine(phase, count):
    phase = phase - jnp.floor((phase + 0.5) * (1.0 / count)) * count
    turn = jnp.abs(phase - 0.5 * count) - 0.25 * count
    x = turn * (2.0 * math.pi / count)
    y = x * x
    total = jnp.full_like(y, -1.0 / math.factorial(11))
    for power, sign in ((9, 1.0), (7, -1.0), (5, 1.0), (3, -1.0), (1, 1.0)):
        total = total * y + sign / math.factorial(power)
    return total * x


def rows_kernel(lats, chans, chunks, columns, mode_ref, spec_ref, legendre_ref, taps_ref,
                w_in_ref, b_in_ref, w_out_ref, field_ref, masked_ref,
                raw, table, stage, coeff, recv, send, got, mix, field, waves, waves_t, filters, perm, marks,
                raw_got, table_sent, field_sent, fwd_sent, fwd_got, bwd_sent, bwd_got):
    slots, span, degrees = raw.shape[1:]
    count = lats * chans
    rows, rows_all = span // count, span * chunks
    depth, width = coeff.shape[3:]
    groups = slots // GROUP
    pair = 2 * GROUP
    lat, chan = lax.axis_index("lat"), lax.axis_index("chan")
    me = lat * chans + chan
    bf16, f32 = jnp.bfloat16, jnp.float32
    across = (((1,), (1,)), ((), ()))

    def fetch(k):
        return pltpu.make_async_copy(
            legendre_ref.at[:, pl.ds(k * span, span), :], raw.at[k % 2], raw_got.at[k % 2])

    def store_table(k):
        part = pl.ds(k * span, span)
        return pltpu.make_async_copy(table.at[:, part, :], masked_ref.at[:, part, :], table_sent.at[k])

    def to_all(block, landing, here, send_sem, recv_sem):
        def to_peer(i, _):
            to = (me + i) % count
            pltpu.make_async_remote_copy(
                src_ref=block(to), dst_ref=landing, send_sem=send_sem, recv_sem=recv_sem,
                device_id=(to // chans, to % chans), device_id_type=pl.DeviceIdType.MESH,
            ).start()
            return 0

        pltpu.make_async_copy(block(me), here, recv_sem).start()
        lax.fori_loop(1, count, to_peer, 0)

    fetch(0).start()
    lane = lax.broadcasted_iota(jnp.int32, (span, degrees), 1)

    def forward(k, _):
        fetch(k).wait()

        @pl.when(k < chunks - 1)
        def _():
            fetch(k + 1).start()

        def group(g, _):
            for i in range(GROUP):
                s = g * GROUP + i
                least = mode_ref[lat * slots + s]
                block = jnp.where(lane >= least, raw[k % 2, s], 0.0).astype(bf16)
                table[s, pl.ds(pl.multiple_of(k * span, span), span), :] = block
                value = lax.dot_general(
                    block, spec_ref[s].reshape(2 * width, degrees), across,
                    preferred_element_type=f32)
                for r in range(2):
                    stage[pl.ds(r * GROUP + i, span, stride=pair), :] = value[:, r * width : (r + 1) * width]
            out = stage[...].astype(bf16).reshape(count, rows, pair, width)
            coeff[k, :, :, pl.ds(pl.multiple_of(g * pair, pair), pair), :] = out
            return 0

        lax.fori_loop(0, groups, group, 0)
        store_table(k).start()
        landing = recv.at[k, :, chan, pl.ds(lat * depth, depth), :]
        to_all(lambda to: coeff.at[k, to], landing, landing, fwd_sent, fwd_got.at[k])
        return 0

    lax.fori_loop(0, chunks, forward, 0)

    factor = columns ** -0.5
    size = lats * depth

    def mark(n, _):
        row = jnp.full((1, width), mode_ref[n], jnp.int32).astype(f32)
        for r in range(2):
            marks[pl.ds(n // GROUP * pair + r * GROUP + n % GROUP, 1), :] = row
        return 0

    lax.fori_loop(0, lats * slots, mark, 0)
    i = lax.broadcasted_iota(jnp.int32, perm.shape, 0)
    j = lax.broadcasted_iota(jnp.int32, perm.shape, 1)
    perm[...] = jnp.where(j == i % width * 2 + i // width, 1.0, 0.0).astype(bf16)

    def wave_rows(n, _):
        here = pl.ds(pl.multiple_of(n * LANES, LANES), LANES)
        k = lax.broadcasted_iota(jnp.int32, (LANES, columns), 0) + n * LANES
        p = lax.broadcasted_iota(jnp.int32, (LANES, columns), 1)
        quarter = (k // GROUP) % 2 * (columns // 4)
        phase = marks[here, :1] * p.astype(f32) + quarter.astype(f32)
        waves[here, :] = (cosine(phase, columns) * factor).astype(bf16)
        return 0

    lax.fori_loop(0, size // LANES, wave_rows, 0)

    line = jnp.concatenate(
        [jnp.transpose(marks[n * LANES : (n + 1) * LANES, :LANES])[:1] for n in range(size // LANES)], axis=1)

    def wave_columns(n, _):
        here = pl.ds(pl.multiple_of(n * LANES, LANES), LANES)
        p = lax.broadcasted_iota(jnp.int32, (LANES, size), 0) + n * LANES
        k = lax.broadcasted_iota(jnp.int32, (LANES, size), 1)
        quarter = (k // GROUP) % 2 * (columns // 4)
        phase = line * p.astype(f32) + quarter.astype(f32)
        waves_t[here, :] = (cosine(phase, columns) * factor).astype(bf16)
        return 0

    lax.fori_loop(0, columns // LANES, wave_columns, 0)

    angle = jnp.concatenate(
        [marks[pl.ds(lat * depth + g * pair, GROUP), :] for g in range(groups)], axis=0)
    cos, minus_sin = cosine(angle, columns), cosine(angle + 0.25 * columns, columns)
    for i in range(3):
        left, here, right = (taps_ref[3 * i + j : 3 * i + j + 1, :] for j in range(3))
        filters[2 * i] = here + (left + right) * cos + (1.0 if i == 1 else 0.0)
        filters[2 * i + 1] = (left - right) * minus_sin
    filters[6] = cosine(angle * (columns // 2), columns)

    def one_chunk(k, _):
        pltpu.make_async_copy(recv.at[k], recv.at[k], fwd_got.at[k]).wait()

        def one_row(j, _):
            merged = jnp.concatenate([recv[k, j, i] for i in range(chans)], axis=1)
            grid = jnp.dot(waves_t[...], merged, preferred_element_type=f32).astype(bf16)
            pre = lax.dot_general(grid, w_in_ref[...], across, preferred_element_type=f32) + b_in_ref[...]
            hidden = jax.nn.gelu(pre, approximate=True).astype(bf16)
            branch = lax.dot_general(hidden, w_out_ref[...], across, preferred_element_type=f32)
            mixed = (grid.astype(f32) + branch).astype(bf16)
            modes = jnp.dot(waves[...], mixed, preferred_element_type=f32).astype(bf16)
            for i in range(chans):
                send[k, j, i] = modes[:, i * width : (i + 1) * width]
            return 0

        lax.fori_loop(0, rows, one_row, 0)
        landing = got.at[pl.ds(1 + k * span + me * rows, rows)]
        to_all(
            lambda to: send.at[k, :, to % chans, pl.ds((to // chans) * depth, depth), :],
            landing, landing, bwd_sent, bwd_got.at[k])
        return 0

    lax.fori_loop(0, chunks, one_chunk, 0)

    most = mix.shape[0] // pair
    lag = most - span
    copies = []
    for k in range(chunks):
        arrived = got.at[pl.ds(1 + k * span, span)]
        pltpu.make_async_copy(arrived, arrived, bwd_got.at[k]).wait()
        low = max(k * span - lag, 0)
        high = rows_all if k == chunks - 1 else (k + 1) * span - lag

        def group(g, _):
            part = pl.ds(pl.multiple_of(g * pair, pair), pair)
            own = pl.ds(pl.multiple_of(g * GROUP, GROUP), GROUP)
            fs = [filters[i, own, :] for i in range(7)]

            def load(t):
                both = got[t, part, :].astype(f32)
                return both[:GROUP], both[GROUP:]

            both_signs = jnp.concatenate([fs[6], fs[6]], axis=0)
            if k == 0:
                got[0, part, :] = (got[1, part, :].astype(f32) * both_signs).astype(bf16)
            if k == chunks - 1:
                got[rows_all + 1, part, :] = (got[rows_all, part, :].astype(f32) * both_signs).astype(bf16)

            def some_rows(n, held):
                for u in range(GROUP):
                    t = n * GROUP + u
                    three = (*held, load(low + t + 2))
                    real = imag = 0.0
                    for i, (x, y) in enumerate(three):
                        real = real + fs[2 * i] * x - fs[2 * i + 1] * y
                        imag = imag + fs[2 * i] * y + fs[2 * i + 1] * x
                    mix[pl.ds(t, GROUP, stride=most), :] = real
                    mix[pl.ds(GROUP * most + t, GROUP, stride=most), :] = imag
                    held = three[1:]
                return held

            lax.fori_loop(0, (high - low) // GROUP, some_rows, (load(low), load(low + 1)))
            for i in range(GROUP):
                parts = [mix[pl.ds((r * GROUP + i) * most, high - low), :] for r in range(2)]
                both = jnp.concatenate(parts, axis=1).astype(bf16)
                field[g * GROUP + i, low:high, :] = jnp.dot(
                    both, perm[...], preferred_element_type=f32).astype(bf16)
            return 0

        lax.fori_loop(0, groups, group, 0)
        copy = pltpu.make_async_copy(
            field.at[:, low:high, :], field_ref.at[:, low:high, :], field_sent.at[k])
        copy.start()
        copies.append(copy)

    for k, copy in enumerate(copies):
        copy.wait()
        store_table(k).wait()
    for ref, sem in ((coeff, fwd_sent), (coeff, bwd_sent)):
        away = ref.at[:, pl.ds(0, count - 1)]
        pltpu.make_async_copy(away, away, sem).wait()


def degrees_kernel(field_ref, masked_ref, out_ref):
    for s in range(field_ref.shape[0]):
        out = lax.dot_general(
            field_ref[s], masked_ref[s], (((0,), (0,)), ((), ())), preferred_element_type=jnp.float32)
        out_ref[s] = out.astype(jnp.bfloat16).reshape(out_ref.shape[1:])


def on_device_rows(spec_in, legendre, mode_slot, w_in, b_in, w_out, kernel):
    lats, chans = lax.axis_size("lat"), lax.axis_size("chan")
    count = lats * chans
    slots, rows_all, degrees = legendre.shape
    width = spec_in.shape[2]
    own_rows = rows_all // count
    chunks = next(k for k in (4, 3, 2, 1) if own_rows % k == 0 and rows_all // k % 16 == 0)
    rows, span = own_rows // chunks, rows_all // chunks
    columns, groups, depth = NLON, slots // GROUP, 2 * slots
    hbm, vmem = pl.BlockSpec(memory_space=pl.ANY), pl.BlockSpec(memory_space=pltpu.VMEM)
    smem = pl.BlockSpec(memory_space=pltpu.SMEM)
    lag = 16 if chunks > 1 else 0
    bf16, f32 = jnp.bfloat16, jnp.float32
    field, masked = pl.pallas_call(
        functools.partial(rows_kernel, lats, chans, chunks, columns),
        out_shape=(
            jax.ShapeDtypeStruct((slots, rows_all, 2 * width), bf16),
            jax.ShapeDtypeStruct((slots, rows_all, degrees), bf16),
        ),
        in_specs=[smem, vmem, hbm] + [vmem] * 4,
        out_specs=(hbm, hbm),
        scratch_shapes=[
            pltpu.VMEM((2, slots, span, degrees), f32),
            pltpu.VMEM((slots, rows_all, degrees), bf16),
            pltpu.VMEM((span * 2 * GROUP, width), f32),
            pltpu.VMEM((chunks, count, rows, depth, width), bf16),
            pltpu.VMEM((chunks, rows, chans, lats * depth, width), bf16),
            pltpu.VMEM((chunks, rows, chans, lats * depth, width), bf16),
            pltpu.VMEM((rows_all + 2, depth, width), bf16),
            pltpu.VMEM(((span + lag) * 2 * GROUP, width), f32),
            pltpu.VMEM((slots, rows_all, 2 * width), bf16),
            pltpu.VMEM((lats * depth, columns), bf16),
            pltpu.VMEM((columns, lats * depth), bf16),
            pltpu.VMEM((7, slots, width), f32),
            pltpu.VMEM((2 * width, 2 * width), bf16),
            pltpu.VMEM((lats * depth, width), f32),
            pltpu.SemaphoreType.DMA((2,)),
            pltpu.SemaphoreType.DMA((chunks,)),
            pltpu.SemaphoreType.DMA((chunks,)),
            pltpu.SemaphoreType.DMA,
            pltpu.SemaphoreType.DMA((chunks,)),
            pltpu.SemaphoreType.DMA,
            pltpu.SemaphoreType.DMA((chunks,)),
        ],
        compiler_params=pltpu.CompilerParams(vmem_limit_bytes=61 * 1024 * 1024, has_side_effects=True),
        name="rows",
    )(mode_slot, jnp.swapaxes(spec_in[:, 0], 1, 2), legendre, kernel.T, w_in, b_in[None, :], w_out)
    some = next(n for n in (4, 3, 2, 1) if slots % n == 0)
    out = pl.pallas_call(
        degrees_kernel,
        grid=(slots // some,),
        out_shape=jax.ShapeDtypeStruct((slots, width, 2, degrees), bf16),
        in_specs=[
            pl.BlockSpec((some, rows_all, 2 * width), lambda n: (n, 0, 0)),
            pl.BlockSpec((some, rows_all, degrees), lambda n: (n, 0, 0)),
        ],
        out_specs=pl.BlockSpec((some, width, 2, degrees), lambda n: (n, 0, 0, 0)),
        compiler_params=pltpu.CompilerParams(vmem_limit_bytes=61 * 1024 * 1024),
        name="degrees",
    )(field, masked)
    return out[:, None]


def solution(mesh):
    in_specs = (
        P("lat", None, "chan", None, None),
        P("lat", None, None),
        P(),
        P(),
        P(),
        P(),
        P("chan", None),
    )
    out_specs = P("lat", None, "chan", None, None)
    count = mesh.shape["lat"] * mesh.shape["chan"]

    def call(spec_in, legendre, *rest):
        samples, rows_all = spec_in.shape[1], legendre.shape[1]
        slots = spec_in.shape[0] // mesh.shape["lat"]
        by_rows = samples == 1 and rows_all % count == 0 and slots % GROUP == 0
        body = on_device_rows if by_rows else on_device
        return jax.shard_map(
            body, mesh=mesh, in_specs=in_specs, out_specs=out_specs, check_vma=False
        )(spec_in, legendre, *rest)

    return call
```

```python
import functools
import math

import jax
import jax.numpy as jnp
from jax import lax
from jax.experimental import pallas as pl
from jax.experimental.pallas import tpu as pltpu
from jax.sharding import PartitionSpec as P

NLON = 768


def with_halo(array, sides, width):
    for axis, dim in sides:
        count, length = (lax.axis_size(axis), array.shape[dim])
        up = [(i, (i + 1) % count) for i in range(count - 1)]
        down = [(j, i) for i, j in up]
        last = lax.slice_in_dim(array, length - width, length, axis=dim)
        first = lax.slice_in_dim(array, 0, width, axis=dim)
        before = lax.ppermute(last, axis, up)
        after = lax.ppermute(first, axis, down)
        array = jnp.concatenate([before, array, after], axis=dim)
    return array


def wave_table(modes, count):
    columns = jnp.arange(count, dtype=jnp.int32)
    phase = modes[:, None] * columns[None, :] % count
    angle = phase.astype(jnp.float32) * (2.0 * math.pi / count)
    factor = count ** (-0.5)
    return jnp.stack([jnp.cos(angle) * factor, -jnp.sin(angle) * factor], axis=1)


def on_device(spec_in, legendre, mode_slot, w_in, b_in, w_out, kernel):
    high = lax.Precision.HIGHEST
    slots_here = legendre.shape[0]
    lat_index = lax.axis_index("lat")
    local_modes = lax.dynamic_slice_in_dim(mode_slot, lat_index * slots_here, slots_here)
    degrees = jnp.arange(legendre.shape[2], dtype=jnp.int32)
    masked = jnp.where(
        degrees[None, None, :] >= local_modes[:, None, None], legendre, jnp.float32(0.0)
    )
    waves = wave_table(mode_slot, NLON)
    coeff = jnp.einsum("sbcrl,stl->sbcrt", spec_in.astype(jnp.float32), masked, precision=high)
    grid = jnp.einsum(
        "sbcrt,srp->btcp",
        lax.all_to_all(coeff, "lat", split_axis=4, concat_axis=0, tiled=True),
        waves,
        precision=high,
    ).astype(jnp.bfloat16)
    batch, rows_here, chan_here, columns = grid.shape
    whole = lax.all_gather(grid, "chan", axis=2, tiled=True)
    chan_index = lax.axis_index("chan")
    w_local = lax.dynamic_slice_in_dim(w_out, chan_index * chan_here, chan_here, 0)
    pre = jnp.einsum("hc,btcp->bthp", w_in, whole, preferred_element_type=jnp.float32)
    hidden = jax.nn.gelu(pre + b_in[None, None, :, None], approximate=True).astype(jnp.bfloat16)
    branch = jnp.einsum("ch,bthp->btcp", w_local, hidden, preferred_element_type=jnp.float32)
    mixed = (grid.astype(jnp.float32) + branch).astype(jnp.bfloat16)
    half = columns // 2
    last_row = lax.axis_size("lat") - 1
    padded = with_halo(mixed, (("lat", 1),), 1)
    upper = jnp.where(lat_index == 0, jnp.roll(mixed[:, 0:1], half, axis=3), padded[:, 0:1])
    lower = jnp.where(lat_index == last_row, jnp.roll(mixed[:, -1:], half, axis=3), padded[:, -1:])
    stacked = jnp.concatenate([upper, padded[:, 1:-1], lower], axis=1).astype(jnp.float32)
    wide = mixed.astype(jnp.float32)
    conv = jnp.zeros_like(wide)
    for i in range(3):
        band = stacked[:, i : i + rows_here]
        for j in range(3):
            conv = conv + kernel[:, 3 * i + j][None, None, :, None] * jnp.roll(band, 1 - j, axis=3)
    field = wide + conv
    modes = jnp.einsum("btcp,srp->sbcrt", field, waves, precision=high)
    return jnp.einsum(
        "sbcrt,stl->sbcrl",
        lax.all_to_all(modes, "lat", split_axis=0, concat_axis=4, tiled=True),
        masked,
        precision=high,
    ).astype(jnp.bfloat16)


GROUP = 8
LANES = 128


def cosine(phase, count):
    phase = phase - jnp.floor((phase + 0.5) * (1.0 / count)) * count
    turn = jnp.abs(phase - 0.5 * count) - 0.25 * count
    x = turn * (2.0 * math.pi / count)
    y = x * x
    total = jnp.full_like(y, -1.0 / math.factorial(11))
    for power, sign in ((9, 1.0), (7, -1.0), (5, 1.0), (3, -1.0), (1, 1.0)):
        total = total * y + sign / math.factorial(power)
    return total * x


def rows_kernel(lats, chans, chunks, columns, mode_ref, spec_ref, legendre_ref, taps_ref,
                w_in_ref, b_in_ref, w_out_ref, out_ref,
                raw, spec, table, stage, coeff, recv, send, got, mix, field, waves, waves_t, filters, perm, perm_t, marks,
                raw_got, spec_got, out_sent, fwd_sent, fwd_got, bwd_sent, bwd_got):
    span, degrees = raw.shape[2:]
    slots = table.shape[0]
    count = lats * chans
    rows, rows_all = span // count, span * chunks
    depth, width = coeff.shape[3:]
    groups = slots // GROUP
    pair = 2 * GROUP
    lat, chan = lax.axis_index("lat"), lax.axis_index("chan")
    me = lat * chans + chan
    bf16, f32 = jnp.bfloat16, jnp.float32
    across = (((1,), (1,)), ((), ()))

    def fetch(n):
        return pltpu.make_async_copy(
            legendre_ref.at[pl.ds(n % groups * GROUP, GROUP), pl.ds(n // groups * span, span), :],
            raw.at[n % 2], raw_got.at[n % 2])

    def fetch_spec(g):
        part = pl.ds(g * GROUP, GROUP)
        return pltpu.make_async_copy(spec_ref.at[part], spec.at[part], spec_got.at[g])

    def to_all(block, landing, here, send_sem, recv_sem):
        def to_peer(i, _):
            to = (me + i) % count
            pltpu.make_async_remote_copy(
                src_ref=block(to), dst_ref=landing, send_sem=send_sem, recv_sem=recv_sem,
                device_id=(to // chans, to % chans), device_id_type=pl.DeviceIdType.MESH,
            ).start()
            return 0

        pltpu.make_async_copy(block(me), here, recv_sem).start()
        lax.fori_loop(1, count, to_peer, 0)

    fetch(0).start()
    for g in range(groups):
        fetch_spec(g).start()
    i = lax.broadcasted_iota(jnp.int32, perm.shape, 0)
    j = lax.broadcasted_iota(jnp.int32, perm.shape, 1)
    perm[...] = jnp.where(j == i % width * 2 + i // width, 1.0, 0.0).astype(bf16)
    perm_t[...] = jnp.where(i == j % width * 2 + j // width, 1.0, 0.0).astype(bf16)
    lane = lax.broadcasted_iota(jnp.int32, (span, degrees), 1)

    def forward(n, _):
        k, g = n // groups, n % groups
        fetch(n).wait()

        @pl.when(n < chunks * groups - 1)
        def _():
            fetch(n + 1).start()

        @pl.when(k == 0)
        def _():
            fetch_spec(g).wait()

        for i in range(GROUP):
            s = g * GROUP + i
            least = mode_ref[lat * slots + s]
            block = jnp.where(lane >= least, raw[n % 2, i], 0.0).astype(bf16)
            table[s, pl.ds(pl.multiple_of(k * span, span), span), :] = block
            value = lax.dot_general(
                block, spec[s].reshape(2 * width, degrees), across, preferred_element_type=f32)
            value = jnp.dot(value.astype(bf16), perm_t[...], preferred_element_type=f32)
            for r in range(2):
                stage[pl.ds(r * GROUP + i, span, stride=pair), :] = value[:, r * width : (r + 1) * width]
        part = pl.ds(pl.multiple_of(g * pair, pair), pair)
        coeff[k, :, :, part, :] = stage[...].astype(bf16).reshape(count, rows, pair, width)

        @pl.when(k == 0)
        def _():
            landing = recv.at[k, :, chan, pl.ds(lat * depth + g * pair, pair), :]
            to_all(lambda to: coeff.at[k, to, :, part, :], landing, landing, fwd_sent, fwd_got.at[k])

        @pl.when((k > 0) & (g == groups - 1))
        def _():
            landing = recv.at[k, :, chan, pl.ds(lat * depth, depth), :]
            to_all(lambda to: coeff.at[k, to], landing, landing, fwd_sent, fwd_got.at[k])

        return 0

    lax.fori_loop(0, chunks * groups, forward, 0)

    factor = columns ** -0.5
    size = lats * depth

    def mark(n, _):
        row = jnp.full((1, width), mode_ref[n], jnp.int32).astype(f32)
        for r in range(2):
            marks[pl.ds(n // GROUP * pair + r * GROUP + n % GROUP, 1), :] = row
        return 0

    lax.fori_loop(0, lats * slots, mark, 0)
    def wave_rows(n, _):
        here = pl.ds(pl.multiple_of(n * LANES, LANES), LANES)
        k = lax.broadcasted_iota(jnp.int32, (LANES, columns), 0) + n * LANES
        p = lax.broadcasted_iota(jnp.int32, (LANES, columns), 1)
        quarter = (k // GROUP) % 2 * (columns // 4)
        phase = marks[here, :1] * p.astype(f32) + quarter.astype(f32)
        waves[here, :] = (cosine(phase, columns) * factor).astype(bf16)
        return 0

    lax.fori_loop(0, size // LANES, wave_rows, 0)

    line = jnp.concatenate(
        [jnp.transpose(marks[n * LANES : (n + 1) * LANES, :LANES])[:1] for n in range(size // LANES)], axis=1)

    def wave_columns(n, _):
        here = pl.ds(pl.multiple_of(n * LANES, LANES), LANES)
        p = lax.broadcasted_iota(jnp.int32, (LANES, size), 0) + n * LANES
        k = lax.broadcasted_iota(jnp.int32, (LANES, size), 1)
        quarter = (k // GROUP) % 2 * (columns // 4)
        phase = line * p.astype(f32) + quarter.astype(f32)
        waves_t[here, :] = (cosine(phase, columns) * factor).astype(bf16)
        return 0

    lax.fori_loop(0, columns // LANES, wave_columns, 0)

    angle = jnp.concatenate(
        [marks[pl.ds(lat * depth + g * pair, GROUP), :] for g in range(groups)], axis=0)
    cos, minus_sin = cosine(angle, columns), cosine(angle + 0.25 * columns, columns)
    for i in range(3):
        left, here, right = (taps_ref[3 * i + j : 3 * i + j + 1, :] for j in range(3))
        filters[2 * i] = here + (left + right) * cos + (1.0 if i == 1 else 0.0)
        filters[2 * i + 1] = (left - right) * minus_sin
    filters[6] = cosine(angle * (columns // 2), columns)

    def one_chunk(k, _):
        pltpu.make_async_copy(recv.at[k], recv.at[k], fwd_got.at[k]).wait()

        def one_row(j, _):
            merged = jnp.concatenate([recv[k, j, i] for i in range(chans)], axis=1)
            grid = jnp.dot(waves_t[...], merged, preferred_element_type=f32).astype(bf16)
            pre = lax.dot_general(grid, w_in_ref[...], across, preferred_element_type=f32) + b_in_ref[...]
            hidden = jax.nn.gelu(pre, approximate=True).astype(bf16)
            branch = lax.dot_general(hidden, w_out_ref[...], across, preferred_element_type=f32)
            mixed = (grid.astype(f32) + branch).astype(bf16)
            modes = jnp.dot(waves[...], mixed, preferred_element_type=f32).astype(bf16)
            for i in range(chans):
                send[k, j, i] = modes[:, i * width : (i + 1) * width]
            return 0

        lax.fori_loop(0, rows, one_row, 0)
        landing = pl.ds(1 + k * span + me * rows, rows)

        @pl.when(k < chunks - 1)
        def _():
            here = got.at[landing]
            to_all(
                lambda to: send.at[k, :, to % chans, pl.ds((to // chans) * depth, depth), :],
                here, here, bwd_sent, bwd_got.at[k])

        @pl.when(k == chunks - 1)
        def _():
            def group(g, _):
                here = got.at[landing, pl.ds(g * pair, pair), :]
                to_all(
                    lambda to: send.at[k, :, to % chans, pl.ds((to // chans) * depth + g * pair, pair), :],
                    here, here, bwd_sent, bwd_got.at[k + g])
                return 0

            lax.fori_loop(0, groups, group, 0)

        return 0

    lax.fori_loop(0, chunks, one_chunk, 0)

    most = mix.shape[0] // pair
    lag = most - span

    def result(g):
        part = pl.ds(g * GROUP, GROUP)
        return pltpu.make_async_copy(spec.at[part], out_ref.at[part], out_sent.at[g])

    for k in range(chunks):
        arrived = pl.ds(1 + k * span, span)
        if k < chunks - 1:
            pltpu.make_async_copy(got.at[arrived], got.at[arrived], bwd_got.at[k]).wait()
        low = max(k * span - lag, 0)
        high = rows_all if k == chunks - 1 else (k + 1) * span - lag

        def group(g, _):
            part = pl.ds(pl.multiple_of(g * pair, pair), pair)
            if k == chunks - 1:
                last = got.at[arrived, part, :]
                pltpu.make_async_copy(last, last, bwd_got.at[k + g]).wait()
            own = pl.ds(pl.multiple_of(g * GROUP, GROUP), GROUP)
            fs = [filters[i, own, :] for i in range(7)]

            def load(t):
                both = got[t, part, :].astype(f32)
                return both[:GROUP], both[GROUP:]

            both_signs = jnp.concatenate([fs[6], fs[6]], axis=0)
            if k == 0:
                got[0, part, :] = (got[1, part, :].astype(f32) * both_signs).astype(bf16)
            if k == chunks - 1:
                got[rows_all + 1, part, :] = (got[rows_all, part, :].astype(f32) * both_signs).astype(bf16)

            def some_rows(n, held):
                for u in range(GROUP):
                    t = n * GROUP + u
                    three = (*held, load(low + t + 2))
                    real = imag = 0.0
                    for i, (x, y) in enumerate(three):
                        real = real + fs[2 * i] * x - fs[2 * i + 1] * y
                        imag = imag + fs[2 * i] * y + fs[2 * i + 1] * x
                    mix[pl.ds(t, GROUP, stride=most), :] = real
                    mix[pl.ds(GROUP * most + t, GROUP, stride=most), :] = imag
                    held = three[1:]
                return held

            lax.fori_loop(0, (high - low) // GROUP, some_rows, (load(low), load(low + 1)))
            for i in range(GROUP):
                parts = [mix[pl.ds((r * GROUP + i) * most, high - low), :] for r in range(2)]
                both = jnp.concatenate(parts, axis=1).astype(bf16)
                field[g * GROUP + i, low:high, :] = jnp.dot(
                    both, perm[...], preferred_element_type=f32).astype(bf16)
            if k == chunks - 1:
                for i in range(GROUP):
                    s = g * GROUP + i
                    out = lax.dot_general(
                        field[s], table[s], (((0,), (0,)), ((), ())), preferred_element_type=f32)
                    spec[s] = out.astype(bf16).reshape(spec.shape[1:])
                result(g).start()
            return 0

        lax.fori_loop(0, groups, group, 0)

    for g in range(groups):
        result(g).wait()
    for ref, sem in ((coeff, fwd_sent), (coeff, bwd_sent)):
        away = ref.at[:, pl.ds(0, count - 1)]
        pltpu.make_async_copy(away, away, sem).wait()


def hand_on(pieces, in_ref, out_ref, held, got, sent):
    size = in_ref.shape[0] // pieces
    parts = [pl.ds(i * size, size) for i in range(pieces)]
    inward = [pltpu.make_async_copy(in_ref.at[p], held.at[p], got.at[i]) for i, p in enumerate(parts)]
    outward = [pltpu.make_async_copy(held.at[p], out_ref.at[p], sent.at[i]) for i, p in enumerate(parts)]
    for copy in inward:
        copy.start()
    for before, after in zip(inward, outward):
        before.wait()
        after.start()
    for copy in outward:
        copy.wait()


def on_device_rows(spec_in, legendre, mode_slot, w_in, b_in, w_out, kernel):
    lats, chans = lax.axis_size("lat"), lax.axis_size("chan")
    count = lats * chans
    slots, rows_all, degrees = legendre.shape
    width = spec_in.shape[2]
    own_rows = rows_all // count
    chunks = next(k for k in (4, 3, 2, 1) if own_rows % k == 0 and rows_all // k % 16 == 0)
    rows, span = own_rows // chunks, rows_all // chunks
    columns, groups, depth = NLON, slots // GROUP, 2 * slots
    hbm, vmem = pl.BlockSpec(memory_space=pl.ANY), pl.BlockSpec(memory_space=pltpu.VMEM)
    smem = pl.BlockSpec(memory_space=pltpu.SMEM)
    lag = 16 if chunks > 1 else 0
    bf16, f32 = jnp.bfloat16, jnp.float32
    out = pl.pallas_call(
        functools.partial(rows_kernel, lats, chans, chunks, columns),
        out_shape=jax.ShapeDtypeStruct((slots, width, 2, degrees), bf16),
        in_specs=[smem] + [hbm] * 2 + [vmem] * 4,
        out_specs=hbm,
        scratch_shapes=[
            pltpu.VMEM((2, GROUP, span, degrees), f32),
            pltpu.VMEM((slots, width, 2, degrees), bf16),
            pltpu.VMEM((slots, rows_all, degrees), bf16),
            pltpu.VMEM((span * 2 * GROUP, width), f32),
            pltpu.VMEM((chunks, count, rows, depth, width), bf16),
            pltpu.VMEM((chunks, rows, chans, lats * depth, width), bf16),
            pltpu.VMEM((chunks, rows, chans, lats * depth, width), bf16),
            pltpu.VMEM((rows_all + 2, depth, width), bf16),
            pltpu.VMEM(((span + lag) * 2 * GROUP, width), f32),
            pltpu.VMEM((slots, rows_all, 2 * width), bf16),
            pltpu.VMEM((lats * depth, columns), bf16),
            pltpu.VMEM((columns, lats * depth), bf16),
            pltpu.VMEM((7, slots, width), f32),
            pltpu.VMEM((2 * width, 2 * width), bf16),
            pltpu.VMEM((2 * width, 2 * width), bf16),
            pltpu.VMEM((lats * depth, width), f32),
            pltpu.SemaphoreType.DMA((2,)),
            pltpu.SemaphoreType.DMA((groups,)),
            pltpu.SemaphoreType.DMA((groups,)),
            pltpu.SemaphoreType.DMA,
            pltpu.SemaphoreType.DMA((chunks,)),
            pltpu.SemaphoreType.DMA,
            pltpu.SemaphoreType.DMA((chunks + groups - 1,)),
        ],
        compiler_params=pltpu.CompilerParams(vmem_limit_bytes=61 * 1024 * 1024, has_side_effects=True),
        name="rows",
    )(mode_slot, spec_in[:, 0], legendre, kernel.T, w_in, b_in[None, :], w_out)
    pieces = next(n for n in (8, 6, 4, 3, 2, 1) if slots % n == 0)
    out = pl.pallas_call(
        functools.partial(hand_on, pieces),
        out_shape=jax.ShapeDtypeStruct(out.shape, bf16),
        in_specs=[hbm],
        out_specs=hbm,
        scratch_shapes=[
            pltpu.VMEM(out.shape, bf16),
            pltpu.SemaphoreType.DMA((pieces,)),
            pltpu.SemaphoreType.DMA((pieces,)),
        ],
        compiler_params=pltpu.CompilerParams(vmem_limit_bytes=61 * 1024 * 1024),
        name="hand_on",
    )(out)
    return out[:, None]


def solution(mesh):
    in_specs = (
        P("lat", None, "chan", None, None),
        P("lat", None, None),
        P(),
        P(),
        P(),
        P(),
        P("chan", None),
    )
    out_specs = P("lat", None, "chan", None, None)
    count = mesh.shape["lat"] * mesh.shape["chan"]

    def call(spec_in, legendre, *rest):
        samples, rows_all = spec_in.shape[1], legendre.shape[1]
        slots = spec_in.shape[0] // mesh.shape["lat"]
        by_rows = samples == 1 and rows_all % count == 0 and slots % GROUP == 0
        body = on_device_rows if by_rows else on_device
        return jax.shard_map(
            body, mesh=mesh, in_specs=in_specs, out_specs=out_specs, check_vma=False
        )(spec_in, legendre, *rest)

    return call
```

```python
import functools
import math

import jax
import jax.numpy as jnp
from jax import lax
from jax.experimental import pallas as pl
from jax.experimental.pallas import tpu as pltpu
from jax.sharding import PartitionSpec as P

NLON = 768


def with_halo(array, sides, width):
    for axis, dim in sides:
        count, length = (lax.axis_size(axis), array.shape[dim])
        up = [(i, (i + 1) % count) for i in range(count - 1)]
        down = [(j, i) for i, j in up]
        last = lax.slice_in_dim(array, length - width, length, axis=dim)
        first = lax.slice_in_dim(array, 0, width, axis=dim)
        before = lax.ppermute(last, axis, up)
        after = lax.ppermute(first, axis, down)
        array = jnp.concatenate([before, array, after], axis=dim)
    return array


def wave_table(modes, count):
    columns = jnp.arange(count, dtype=jnp.int32)
    phase = modes[:, None] * columns[None, :] % count
    angle = phase.astype(jnp.float32) * (2.0 * math.pi / count)
    factor = count ** (-0.5)
    return jnp.stack([jnp.cos(angle) * factor, -jnp.sin(angle) * factor], axis=1)


def on_device(spec_in, legendre, mode_slot, w_in, b_in, w_out, kernel):
    high = lax.Precision.HIGHEST
    slots_here = legendre.shape[0]
    lat_index = lax.axis_index("lat")
    local_modes = lax.dynamic_slice_in_dim(mode_slot, lat_index * slots_here, slots_here)
    degrees = jnp.arange(legendre.shape[2], dtype=jnp.int32)
    masked = jnp.where(
        degrees[None, None, :] >= local_modes[:, None, None], legendre, jnp.float32(0.0)
    )
    waves = wave_table(mode_slot, NLON)
    coeff = jnp.einsum("sbcrl,stl->sbcrt", spec_in.astype(jnp.float32), masked, precision=high)
    grid = jnp.einsum(
        "sbcrt,srp->btcp",
        lax.all_to_all(coeff, "lat", split_axis=4, concat_axis=0, tiled=True),
        waves,
        precision=high,
    ).astype(jnp.bfloat16)
    batch, rows_here, chan_here, columns = grid.shape
    whole = lax.all_gather(grid, "chan", axis=2, tiled=True)
    chan_index = lax.axis_index("chan")
    w_local = lax.dynamic_slice_in_dim(w_out, chan_index * chan_here, chan_here, 0)
    pre = jnp.einsum("hc,btcp->bthp", w_in, whole, preferred_element_type=jnp.float32)
    hidden = jax.nn.gelu(pre + b_in[None, None, :, None], approximate=True).astype(jnp.bfloat16)
    branch = jnp.einsum("ch,bthp->btcp", w_local, hidden, preferred_element_type=jnp.float32)
    mixed = (grid.astype(jnp.float32) + branch).astype(jnp.bfloat16)
    half = columns // 2
    last_row = lax.axis_size("lat") - 1
    padded = with_halo(mixed, (("lat", 1),), 1)
    upper = jnp.where(lat_index == 0, jnp.roll(mixed[:, 0:1], half, axis=3), padded[:, 0:1])
    lower = jnp.where(lat_index == last_row, jnp.roll(mixed[:, -1:], half, axis=3), padded[:, -1:])
    stacked = jnp.concatenate([upper, padded[:, 1:-1], lower], axis=1).astype(jnp.float32)
    wide = mixed.astype(jnp.float32)
    conv = jnp.zeros_like(wide)
    for i in range(3):
        band = stacked[:, i : i + rows_here]
        for j in range(3):
            conv = conv + kernel[:, 3 * i + j][None, None, :, None] * jnp.roll(band, 1 - j, axis=3)
    field = wide + conv
    modes = jnp.einsum("btcp,srp->sbcrt", field, waves, precision=high)
    return jnp.einsum(
        "sbcrt,stl->sbcrl",
        lax.all_to_all(modes, "lat", split_axis=0, concat_axis=4, tiled=True),
        masked,
        precision=high,
    ).astype(jnp.bfloat16)


GROUP = 8
LANES = 128


def cosine(phase, count):
    phase = phase - jnp.floor((phase + 0.5) * (1.0 / count)) * count
    turn = jnp.abs(phase - 0.5 * count) - 0.25 * count
    x = turn * (2.0 * math.pi / count)
    y = x * x
    total = jnp.full_like(y, -1.0 / math.factorial(11))
    for power, sign in ((9, 1.0), (7, -1.0), (5, 1.0), (3, -1.0), (1, 1.0)):
        total = total * y + sign / math.factorial(power)
    return total * x


def rows_kernel(lats, chans, chunks, columns, mode_ref, spec_ref, legendre_ref, taps_ref,
                w_in_ref, b_in_ref, w_out_ref, out_ref,
                raw, spec, table, stage, coeff, recv, send, got, mix, field, waves, waves_t, filters, perm, perm_t, marks,
                raw_got, spec_got, out_sent, fwd_sent, fwd_got, bwd_sent, bwd_got):
    span, degrees = raw.shape[2:]
    slots = table.shape[0]
    count = lats * chans
    rows, rows_all = span // count, span * chunks
    depth, width = coeff.shape[3:]
    groups = slots // GROUP
    pair = 2 * GROUP
    lat, chan = lax.axis_index("lat"), lax.axis_index("chan")
    me = lat * chans + chan
    bf16, f32 = jnp.bfloat16, jnp.float32
    across = (((1,), (1,)), ((), ()))

    def fetch(n):
        return pltpu.make_async_copy(
            legendre_ref.at[pl.ds(n % groups * GROUP, GROUP), pl.ds(n // groups * span, span), :],
            raw.at[n % 2], raw_got.at[n % 2])

    def fetch_spec(g):
        part = pl.ds(g * GROUP, GROUP)
        return pltpu.make_async_copy(spec_ref.at[part], spec.at[part], spec_got.at[g])

    def to_all(block, landing, here, send_sem, recv_sem):
        def to_peer(i, _):
            to = (me + i) % count
            pltpu.make_async_remote_copy(
                src_ref=block(to), dst_ref=landing, send_sem=send_sem, recv_sem=recv_sem,
                device_id=(to // chans, to % chans), device_id_type=pl.DeviceIdType.MESH,
            ).start()
            return 0

        pltpu.make_async_copy(block(me), here, recv_sem).start()
        lax.fori_loop(1, count, to_peer, 0)

    barrier = pltpu.get_barrier_semaphore()

    def greet(i, _):
        to = (me + i) % count
        pl.semaphore_signal(
            barrier, inc=1, device_id=(to // chans, to % chans), device_id_type=pl.DeviceIdType.MESH)
        return 0

    lax.fori_loop(1, count, greet, 0)
    fetch(0).start()
    for g in range(groups):
        fetch_spec(g).start()
    i = lax.broadcasted_iota(jnp.int32, perm.shape, 0)
    j = lax.broadcasted_iota(jnp.int32, perm.shape, 1)
    perm[...] = jnp.where(j == i % width * 2 + i // width, 1.0, 0.0).astype(bf16)
    perm_t[...] = jnp.where(i == j % width * 2 + j // width, 1.0, 0.0).astype(bf16)
    lane = lax.broadcasted_iota(jnp.int32, (span, degrees), 1)

    def work_out(n):
        k, g = n // groups, n % groups
        fetch(n).wait()

        @pl.when(n < chunks * groups - 1)
        def _():
            fetch(n + 1).start()

        @pl.when(k == 0)
        def _():
            fetch_spec(g).wait()

        for i in range(GROUP):
            s = g * GROUP + i
            least = mode_ref[lat * slots + s]
            block = jnp.where(lane >= least, raw[n % 2, i], 0.0).astype(bf16)
            table[s, pl.ds(pl.multiple_of(k * span, span), span), :] = block
            value = lax.dot_general(
                block, spec[s].reshape(2 * width, degrees), across, preferred_element_type=f32)
            value = jnp.dot(value.astype(bf16), perm_t[...], preferred_element_type=f32)
            for r in range(2):
                stage[pl.ds(r * GROUP + i, span, stride=pair), :] = value[:, r * width : (r + 1) * width]
        part = pl.ds(pl.multiple_of(g * pair, pair), pair)
        coeff[k, :, :, part, :] = stage[...].astype(bf16).reshape(count, rows, pair, width)

    def send_group(g):
        part = pl.ds(g * pair, pair)
        landing = recv.at[0, :, chan, pl.ds(lat * depth + g * pair, pair), :]
        to_all(lambda to: coeff.at[0, to, :, part, :], landing, landing, fwd_sent, fwd_got.at[0])

    work_out(0)
    pl.semaphore_wait(barrier, count - 1)
    send_group(0)

    def forward(n, _):
        k, g = n // groups, n % groups
        work_out(n)

        @pl.when(k == 0)
        def _():
            send_group(g)

        @pl.when((k > 0) & (g == groups - 1))
        def _():
            landing = recv.at[k, :, chan, pl.ds(lat * depth, depth), :]
            to_all(lambda to: coeff.at[k, to], landing, landing, fwd_sent, fwd_got.at[k])

        return 0

    lax.fori_loop(1, chunks * groups, forward, 0)

    factor = columns ** -0.5
    size = lats * depth

    def mark(n, _):
        row = jnp.full((1, width), mode_ref[n], jnp.int32).astype(f32)
        for r in range(2):
            marks[pl.ds(n // GROUP * pair + r * GROUP + n % GROUP, 1), :] = row
        return 0

    lax.fori_loop(0, lats * slots, mark, 0)
    def wave_rows(n, _):
        here = pl.ds(pl.multiple_of(n * LANES, LANES), LANES)
        k = lax.broadcasted_iota(jnp.int32, (LANES, columns), 0) + n * LANES
        p = lax.broadcasted_iota(jnp.int32, (LANES, columns), 1)
        quarter = (k // GROUP) % 2 * (columns // 4)
        phase = marks[here, :1] * p.astype(f32) + quarter.astype(f32)
        waves[here, :] = (cosine(phase, columns) * factor).astype(bf16)
        return 0

    lax.fori_loop(0, size // LANES, wave_rows, 0)

    line = jnp.concatenate(
        [jnp.transpose(marks[n * LANES : (n + 1) * LANES, :LANES])[:1] for n in range(size // LANES)], axis=1)

    def wave_columns(n, _):
        here = pl.ds(pl.multiple_of(n * LANES, LANES), LANES)
        p = lax.broadcasted_iota(jnp.int32, (LANES, size), 0) + n * LANES
        k = lax.broadcasted_iota(jnp.int32, (LANES, size), 1)
        quarter = (k // GROUP) % 2 * (columns // 4)
        phase = line * p.astype(f32) + quarter.astype(f32)
        waves_t[here, :] = (cosine(phase, columns) * factor).astype(bf16)
        return 0

    lax.fori_loop(0, columns // LANES, wave_columns, 0)

    angle = jnp.concatenate(
        [marks[pl.ds(lat * depth + g * pair, GROUP), :] for g in range(groups)], axis=0)
    cos, minus_sin = cosine(angle, columns), cosine(angle + 0.25 * columns, columns)
    for i in range(3):
        left, here, right = (taps_ref[3 * i + j : 3 * i + j + 1, :] for j in range(3))
        filters[2 * i] = here + (left + right) * cos + (1.0 if i == 1 else 0.0)
        filters[2 * i + 1] = (left - right) * minus_sin
    filters[6] = cosine(angle * (columns // 2), columns)

    def one_chunk(k, _):
        pltpu.make_async_copy(recv.at[k], recv.at[k], fwd_got.at[k]).wait()

        def one_row(j, _):
            merged = jnp.concatenate([recv[k, j, i] for i in range(chans)], axis=1)
            grid = jnp.dot(waves_t[...], merged, preferred_element_type=f32).astype(bf16)
            pre = lax.dot_general(grid, w_in_ref[...], across, preferred_element_type=f32) + b_in_ref[...]
            hidden = jax.nn.gelu(pre, approximate=True).astype(bf16)
            branch = lax.dot_general(hidden, w_out_ref[...], across, preferred_element_type=f32)
            mixed = (grid.astype(f32) + branch).astype(bf16)
            modes = jnp.dot(waves[...], mixed, preferred_element_type=f32).astype(bf16)
            for i in range(chans):
                send[k, j, i] = modes[:, i * width : (i + 1) * width]
            return 0

        lax.fori_loop(0, rows, one_row, 0)
        landing = pl.ds(1 + k * span + me * rows, rows)

        @pl.when(k < chunks - 1)
        def _():
            here = got.at[landing]
            to_all(
                lambda to: send.at[k, :, to % chans, pl.ds((to // chans) * depth, depth), :],
                here, here, bwd_sent, bwd_got.at[k])

        @pl.when(k == chunks - 1)
        def _():
            def group(g, _):
                here = got.at[landing, pl.ds(g * pair, pair), :]
                to_all(
                    lambda to: send.at[k, :, to % chans, pl.ds((to // chans) * depth + g * pair, pair), :],
                    here, here, bwd_sent, bwd_got.at[k + g])
                return 0

            lax.fori_loop(0, groups, group, 0)

        return 0

    lax.fori_loop(0, chunks, one_chunk, 0)

    most = mix.shape[0] // pair
    lag = most - span

    def result(g):
        part = pl.ds(g * GROUP, GROUP)
        return pltpu.make_async_copy(spec.at[part], out_ref.at[part], out_sent.at[g])

    for k in range(chunks):
        arrived = pl.ds(1 + k * span, span)
        if k < chunks - 1:
            pltpu.make_async_copy(got.at[arrived], got.at[arrived], bwd_got.at[k]).wait()
        low = max(k * span - lag, 0)
        high = rows_all if k == chunks - 1 else (k + 1) * span - lag

        def group(g, _):
            part = pl.ds(pl.multiple_of(g * pair, pair), pair)
            if k == chunks - 1:
                last = got.at[arrived, part, :]
                pltpu.make_async_copy(last, last, bwd_got.at[k + g]).wait()
            own = pl.ds(pl.multiple_of(g * GROUP, GROUP), GROUP)
            fs = [filters[i, own, :] for i in range(7)]

            def load(t):
                both = got[t, part, :].astype(f32)
                return both[:GROUP], both[GROUP:]

            both_signs = jnp.concatenate([fs[6], fs[6]], axis=0)
            if k == 0:
                got[0, part, :] = (got[1, part, :].astype(f32) * both_signs).astype(bf16)
            if k == chunks - 1:
                got[rows_all + 1, part, :] = (got[rows_all, part, :].astype(f32) * both_signs).astype(bf16)

            def some_rows(n, held):
                for u in range(GROUP):
                    t = n * GROUP + u
                    three = (*held, load(low + t + 2))
                    real = imag = 0.0
                    for i, (x, y) in enumerate(three):
                        real = real + fs[2 * i] * x - fs[2 * i + 1] * y
                        imag = imag + fs[2 * i] * y + fs[2 * i + 1] * x
                    mix[pl.ds(t, GROUP, stride=most), :] = real
                    mix[pl.ds(GROUP * most + t, GROUP, stride=most), :] = imag
                    held = three[1:]
                return held

            lax.fori_loop(0, (high - low) // GROUP, some_rows, (load(low), load(low + 1)))
            for i in range(GROUP):
                parts = [mix[pl.ds((r * GROUP + i) * most, high - low), :] for r in range(2)]
                both = jnp.concatenate(parts, axis=1).astype(bf16)
                field[g * GROUP + i, low:high, :] = jnp.dot(
                    both, perm[...], preferred_element_type=f32).astype(bf16)
            if k == chunks - 1:
                for i in range(GROUP):
                    s = g * GROUP + i
                    out = lax.dot_general(
                        field[s], table[s], (((0,), (0,)), ((), ())), preferred_element_type=f32)
                    spec[s] = out.astype(bf16).reshape(spec.shape[1:])
                result(g).start()
            return 0

        lax.fori_loop(0, groups, group, 0)

    for g in range(groups):
        result(g).wait()
    for ref, sem in ((coeff, fwd_sent), (coeff, bwd_sent)):
        away = ref.at[:, pl.ds(0, count - 1)]
        pltpu.make_async_copy(away, away, sem).wait()


def hand_on(pieces, in_ref, out_ref, held, got, sent):
    size = in_ref.shape[0] // pieces
    parts = [pl.ds(i * size, size) for i in range(pieces)]
    inward = [pltpu.make_async_copy(in_ref.at[p], held.at[p], got.at[i]) for i, p in enumerate(parts)]
    outward = [pltpu.make_async_copy(held.at[p], out_ref.at[p], sent.at[i]) for i, p in enumerate(parts)]
    for copy in inward:
        copy.start()
    for before, after in zip(inward, outward):
        before.wait()
        after.start()
    for copy in outward:
        copy.wait()


def on_device_rows(spec_in, legendre, mode_slot, w_in, b_in, w_out, kernel):
    lats, chans = lax.axis_size("lat"), lax.axis_size("chan")
    count = lats * chans
    slots, rows_all, degrees = legendre.shape
    width = spec_in.shape[2]
    own_rows = rows_all // count
    chunks = next(k for k in (4, 3, 2, 1) if own_rows % k == 0 and rows_all // k % 16 == 0)
    rows, span = own_rows // chunks, rows_all // chunks
    columns, groups, depth = NLON, slots // GROUP, 2 * slots
    hbm, vmem = pl.BlockSpec(memory_space=pl.ANY), pl.BlockSpec(memory_space=pltpu.VMEM)
    smem = pl.BlockSpec(memory_space=pltpu.SMEM)
    lag = 16 if chunks > 1 else 0
    bf16, f32 = jnp.bfloat16, jnp.float32
    out = pl.pallas_call(
        functools.partial(rows_kernel, lats, chans, chunks, columns),
        out_shape=jax.ShapeDtypeStruct((slots, width, 2, degrees), bf16),
        in_specs=[smem] + [hbm] * 2 + [vmem] * 4,
        out_specs=hbm,
        scratch_shapes=[
            pltpu.VMEM((2, GROUP, span, degrees), f32),
            pltpu.VMEM((slots, width, 2, degrees), bf16),
            pltpu.VMEM((slots, rows_all, degrees), bf16),
            pltpu.VMEM((span * 2 * GROUP, width), f32),
            pltpu.VMEM((chunks, count, rows, depth, width), bf16),
            pltpu.VMEM((chunks, rows, chans, lats * depth, width), bf16),
            pltpu.VMEM((chunks, rows, chans, lats * depth, width), bf16),
            pltpu.VMEM((rows_all + 2, depth, width), bf16),
            pltpu.VMEM(((span + lag) * 2 * GROUP, width), f32),
            pltpu.VMEM((slots, rows_all, 2 * width), bf16),
            pltpu.VMEM((lats * depth, columns), bf16),
            pltpu.VMEM((columns, lats * depth), bf16),
            pltpu.VMEM((7, slots, width), f32),
            pltpu.VMEM((2 * width, 2 * width), bf16),
            pltpu.VMEM((2 * width, 2 * width), bf16),
            pltpu.VMEM((lats * depth, width), f32),
            pltpu.SemaphoreType.DMA((2,)),
            pltpu.SemaphoreType.DMA((groups,)),
            pltpu.SemaphoreType.DMA((groups,)),
            pltpu.SemaphoreType.DMA,
            pltpu.SemaphoreType.DMA((chunks,)),
            pltpu.SemaphoreType.DMA,
            pltpu.SemaphoreType.DMA((chunks + groups - 1,)),
        ],
        compiler_params=pltpu.CompilerParams(vmem_limit_bytes=61 * 1024 * 1024, has_side_effects=True, collective_id=0),
        name="rows",
    )(mode_slot, spec_in[:, 0], legendre, kernel.T, w_in, b_in[None, :], w_out)
    pieces = next(n for n in (8, 6, 4, 3, 2, 1) if slots % n == 0)
    out = pl.pallas_call(
        functools.partial(hand_on, pieces),
        out_shape=jax.ShapeDtypeStruct(out.shape, bf16),
        in_specs=[hbm],
        out_specs=hbm,
        scratch_shapes=[
            pltpu.VMEM(out.shape, bf16),
            pltpu.SemaphoreType.DMA((pieces,)),
            pltpu.SemaphoreType.DMA((pieces,)),
        ],
        compiler_params=pltpu.CompilerParams(vmem_limit_bytes=61 * 1024 * 1024),
        name="hand_on",
    )(out)
    return out[:, None]


def solution(mesh):
    in_specs = (
        P("lat", None, "chan", None, None),
        P("lat", None, None),
        P(),
        P(),
        P(),
        P(),
        P("chan", None),
    )
    out_specs = P("lat", None, "chan", None, None)
    count = mesh.shape["lat"] * mesh.shape["chan"]

    def call(spec_in, legendre, *rest):
        samples, rows_all = spec_in.shape[1], legendre.shape[1]
        slots = spec_in.shape[0] // mesh.shape["lat"]
        by_rows = samples == 1 and rows_all % count == 0 and slots % GROUP == 0
        body = on_device_rows if by_rows else on_device
        return jax.shard_map(
            body, mesh=mesh, in_specs=in_specs, out_specs=out_specs, check_vma=False
        )(spec_in, legendre, *rest)

    return call
```

```python
import functools
import math

import jax
import jax.numpy as jnp
from jax import lax
from jax.experimental import pallas as pl
from jax.experimental.pallas import tpu as pltpu
from jax.sharding import PartitionSpec as P

NLON = 768


def with_halo(array, sides, width):
    for axis, dim in sides:
        count, length = (lax.axis_size(axis), array.shape[dim])
        up = [(i, (i + 1) % count) for i in range(count - 1)]
        down = [(j, i) for i, j in up]
        last = lax.slice_in_dim(array, length - width, length, axis=dim)
        first = lax.slice_in_dim(array, 0, width, axis=dim)
        before = lax.ppermute(last, axis, up)
        after = lax.ppermute(first, axis, down)
        array = jnp.concatenate([before, array, after], axis=dim)
    return array


def wave_table(modes, count):
    columns = jnp.arange(count, dtype=jnp.int32)
    phase = modes[:, None] * columns[None, :] % count
    angle = phase.astype(jnp.float32) * (2.0 * math.pi / count)
    factor = count ** (-0.5)
    return jnp.stack([jnp.cos(angle) * factor, -jnp.sin(angle) * factor], axis=1)


def on_device(spec_in, legendre, mode_slot, w_in, b_in, w_out, kernel):
    high = lax.Precision.HIGHEST
    slots_here = legendre.shape[0]
    lat_index = lax.axis_index("lat")
    local_modes = lax.dynamic_slice_in_dim(mode_slot, lat_index * slots_here, slots_here)
    degrees = jnp.arange(legendre.shape[2], dtype=jnp.int32)
    masked = jnp.where(
        degrees[None, None, :] >= local_modes[:, None, None], legendre, jnp.float32(0.0)
    )
    waves = wave_table(mode_slot, NLON)
    coeff = jnp.einsum("sbcrl,stl->sbcrt", spec_in.astype(jnp.float32), masked, precision=high)
    grid = jnp.einsum(
        "sbcrt,srp->btcp",
        lax.all_to_all(coeff, "lat", split_axis=4, concat_axis=0, tiled=True),
        waves,
        precision=high,
    ).astype(jnp.bfloat16)
    batch, rows_here, chan_here, columns = grid.shape
    whole = lax.all_gather(grid, "chan", axis=2, tiled=True)
    chan_index = lax.axis_index("chan")
    w_local = lax.dynamic_slice_in_dim(w_out, chan_index * chan_here, chan_here, 0)
    pre = jnp.einsum("hc,btcp->bthp", w_in, whole, preferred_element_type=jnp.float32)
    hidden = jax.nn.gelu(pre + b_in[None, None, :, None], approximate=True).astype(jnp.bfloat16)
    branch = jnp.einsum("ch,bthp->btcp", w_local, hidden, preferred_element_type=jnp.float32)
    mixed = (grid.astype(jnp.float32) + branch).astype(jnp.bfloat16)
    half = columns // 2
    last_row = lax.axis_size("lat") - 1
    padded = with_halo(mixed, (("lat", 1),), 1)
    upper = jnp.where(lat_index == 0, jnp.roll(mixed[:, 0:1], half, axis=3), padded[:, 0:1])
    lower = jnp.where(lat_index == last_row, jnp.roll(mixed[:, -1:], half, axis=3), padded[:, -1:])
    stacked = jnp.concatenate([upper, padded[:, 1:-1], lower], axis=1).astype(jnp.float32)
    wide = mixed.astype(jnp.float32)
    conv = jnp.zeros_like(wide)
    for i in range(3):
        band = stacked[:, i : i + rows_here]
        for j in range(3):
            conv = conv + kernel[:, 3 * i + j][None, None, :, None] * jnp.roll(band, 1 - j, axis=3)
    field = wide + conv
    modes = jnp.einsum("btcp,srp->sbcrt", field, waves, precision=high)
    return jnp.einsum(
        "sbcrt,stl->sbcrl",
        lax.all_to_all(modes, "lat", split_axis=0, concat_axis=4, tiled=True),
        masked,
        precision=high,
    ).astype(jnp.bfloat16)


GROUP = 8
LANES = 128


def cosine(phase, count):
    phase = phase - jnp.floor((phase + 0.5) * (1.0 / count)) * count
    turn = jnp.abs(phase - 0.5 * count) - 0.25 * count
    x = turn * (2.0 * math.pi / count)
    y = x * x
    total = jnp.full_like(y, -1.0 / math.factorial(11))
    for power, sign in ((9, 1.0), (7, -1.0), (5, 1.0), (3, -1.0), (1, 1.0)):
        total = total * y + sign / math.factorial(power)
    return total * x


def rows_kernel(lats, chans, chunks, columns, mode_ref, spec_ref, legendre_ref, taps_ref,
                w_in_ref, b_in_ref, w_out_ref, out_ref,
                raw, spec, table, stage, coeff, recv, send, got, mix, field, waves, waves_t, filters, perm, perm_t, marks,
                raw_got, spec_got, fwd_sent, fwd_got, bwd_sent, bwd_got):
    span, degrees = raw.shape[2:]
    slots = table.shape[0]
    count = lats * chans
    rows, rows_all = span // count, span * chunks
    depth, width = coeff.shape[3:]
    groups = slots // GROUP
    pair = 2 * GROUP
    lat, chan = lax.axis_index("lat"), lax.axis_index("chan")
    me = lat * chans + chan
    bf16, f32 = jnp.bfloat16, jnp.float32
    across = (((1,), (1,)), ((), ()))

    def fetch(n):
        return pltpu.make_async_copy(
            legendre_ref.at[pl.ds(n % groups * GROUP, GROUP), pl.ds(n // groups * span, span), :],
            raw.at[n % 2], raw_got.at[n % 2])

    def fetch_spec(g):
        part = pl.ds(g * GROUP, GROUP)
        return pltpu.make_async_copy(spec_ref.at[part], spec.at[part], spec_got.at[g])

    def to_all(block, landing, here, send_sem, recv_sem):
        def to_peer(i, _):
            to = (me + i) % count
            pltpu.make_async_remote_copy(
                src_ref=block(to), dst_ref=landing, send_sem=send_sem, recv_sem=recv_sem,
                device_id=(to // chans, to % chans), device_id_type=pl.DeviceIdType.MESH,
            ).start()
            return 0

        pltpu.make_async_copy(block(me), here, recv_sem).start()
        lax.fori_loop(1, count, to_peer, 0)

    barrier = pltpu.get_barrier_semaphore()

    def greet(i, _):
        to = (me + i) % count
        pl.semaphore_signal(
            barrier, inc=1, device_id=(to // chans, to % chans), device_id_type=pl.DeviceIdType.MESH)
        return 0

    lax.fori_loop(1, count, greet, 0)
    fetch(0).start()
    for g in range(groups):
        fetch_spec(g).start()
    i = lax.broadcasted_iota(jnp.int32, perm.shape, 0)
    j = lax.broadcasted_iota(jnp.int32, perm.shape, 1)
    perm[...] = jnp.where(j == i % width * 2 + i // width, 1.0, 0.0).astype(bf16)
    perm_t[...] = jnp.where(i == j % width * 2 + j // width, 1.0, 0.0).astype(bf16)
    lane = lax.broadcasted_iota(jnp.int32, (span, degrees), 1)

    def work_out(n):
        k, g = n // groups, n % groups
        fetch(n).wait()

        @pl.when(n < chunks * groups - 1)
        def _():
            fetch(n + 1).start()

        @pl.when(k == 0)
        def _():
            fetch_spec(g).wait()

        for i in range(GROUP):
            s = g * GROUP + i
            least = mode_ref[lat * slots + s]
            block = jnp.where(lane >= least, raw[n % 2, i], 0.0).astype(bf16)
            table[s, pl.ds(pl.multiple_of(k * span, span), span), :] = block
            value = lax.dot_general(
                block, spec[s].reshape(2 * width, degrees), across, preferred_element_type=f32)
            value = jnp.dot(value.astype(bf16), perm_t[...], preferred_element_type=f32)
            for r in range(2):
                stage[pl.ds(r * GROUP + i, span, stride=pair), :] = value[:, r * width : (r + 1) * width]
        part = pl.ds(pl.multiple_of(g * pair, pair), pair)
        coeff[k, :, :, part, :] = stage[...].astype(bf16).reshape(count, rows, pair, width)

    def send_group(g):
        part = pl.ds(g * pair, pair)
        landing = recv.at[0, :, chan, pl.ds(lat * depth + g * pair, pair), :]
        to_all(lambda to: coeff.at[0, to, :, part, :], landing, landing, fwd_sent, fwd_got.at[0])

    work_out(0)
    pl.semaphore_wait(barrier, count - 1)
    send_group(0)

    def forward(n, _):
        k, g = n // groups, n % groups
        work_out(n)

        @pl.when(k == 0)
        def _():
            send_group(g)

        @pl.when((k > 0) & (g == groups - 1))
        def _():
            landing = recv.at[k, :, chan, pl.ds(lat * depth, depth), :]
            to_all(lambda to: coeff.at[k, to], landing, landing, fwd_sent, fwd_got.at[k])

        return 0

    lax.fori_loop(1, chunks * groups, forward, 0)

    factor = columns ** -0.5
    size = lats * depth

    def mark(n, _):
        row = jnp.full((1, width), mode_ref[n], jnp.int32).astype(f32)
        for r in range(2):
            marks[pl.ds(n // GROUP * pair + r * GROUP + n % GROUP, 1), :] = row
        return 0

    lax.fori_loop(0, lats * slots, mark, 0)
    def wave_rows(n, _):
        here = pl.ds(pl.multiple_of(n * LANES, LANES), LANES)
        k = lax.broadcasted_iota(jnp.int32, (LANES, columns), 0) + n * LANES
        p = lax.broadcasted_iota(jnp.int32, (LANES, columns), 1)
        quarter = (k // GROUP) % 2 * (columns // 4)
        phase = marks[here, :1] * p.astype(f32) + quarter.astype(f32)
        waves[here, :] = (cosine(phase, columns) * factor).astype(bf16)
        return 0

    lax.fori_loop(0, size // LANES, wave_rows, 0)

    line = jnp.concatenate(
        [jnp.transpose(marks[n * LANES : (n + 1) * LANES, :LANES])[:1] for n in range(size // LANES)], axis=1)

    def wave_columns(n, _):
        here = pl.ds(pl.multiple_of(n * LANES, LANES), LANES)
        p = lax.broadcasted_iota(jnp.int32, (LANES, size), 0) + n * LANES
        k = lax.broadcasted_iota(jnp.int32, (LANES, size), 1)
        quarter = (k // GROUP) % 2 * (columns // 4)
        phase = line * p.astype(f32) + quarter.astype(f32)
        waves_t[here, :] = (cosine(phase, columns) * factor).astype(bf16)
        return 0

    lax.fori_loop(0, columns // LANES, wave_columns, 0)

    angle = jnp.concatenate(
        [marks[pl.ds(lat * depth + g * pair, GROUP), :] for g in range(groups)], axis=0)
    cos, minus_sin = cosine(angle, columns), cosine(angle + 0.25 * columns, columns)
    for i in range(3):
        left, here, right = (taps_ref[3 * i + j : 3 * i + j + 1, :] for j in range(3))
        filters[2 * i] = here + (left + right) * cos + (1.0 if i == 1 else 0.0)
        filters[2 * i + 1] = (left - right) * minus_sin
    filters[6] = cosine(angle * (columns // 2), columns)

    def one_chunk(k, _):
        pltpu.make_async_copy(recv.at[k], recv.at[k], fwd_got.at[k]).wait()

        def one_row(j, _):
            merged = jnp.concatenate([recv[k, j, i] for i in range(chans)], axis=1)
            grid = jnp.dot(waves_t[...], merged, preferred_element_type=f32).astype(bf16)
            pre = lax.dot_general(grid, w_in_ref[...], across, preferred_element_type=f32) + b_in_ref[...]
            hidden = jax.nn.gelu(pre, approximate=True).astype(bf16)
            branch = lax.dot_general(hidden, w_out_ref[...], across, preferred_element_type=f32)
            mixed = (grid.astype(f32) + branch).astype(bf16)
            modes = jnp.dot(waves[...], mixed, preferred_element_type=f32).astype(bf16)
            for i in range(chans):
                send[k, j, i] = modes[:, i * width : (i + 1) * width]
            return 0

        lax.fori_loop(0, rows, one_row, 0)
        landing = pl.ds(1 + k * span + me * rows, rows)

        @pl.when(k < chunks - 1)
        def _():
            here = got.at[landing]
            to_all(
                lambda to: send.at[k, :, to % chans, pl.ds((to // chans) * depth, depth), :],
                here, here, bwd_sent, bwd_got.at[k])

        @pl.when(k == chunks - 1)
        def _():
            def group(g, _):
                here = got.at[landing, pl.ds(g * pair, pair), :]
                to_all(
                    lambda to: send.at[k, :, to % chans, pl.ds((to // chans) * depth + g * pair, pair), :],
                    here, here, bwd_sent, bwd_got.at[k + g])
                return 0

            lax.fori_loop(0, groups, group, 0)

        return 0

    lax.fori_loop(0, chunks, one_chunk, 0)

    most = mix.shape[0] // pair
    lag = most - span

    for k in range(chunks):
        arrived = pl.ds(1 + k * span, span)
        if k < chunks - 1:
            pltpu.make_async_copy(got.at[arrived], got.at[arrived], bwd_got.at[k]).wait()
        low = max(k * span - lag, 0)
        high = rows_all if k == chunks - 1 else (k + 1) * span - lag

        def group(g, _):
            part = pl.ds(pl.multiple_of(g * pair, pair), pair)
            if k == chunks - 1:
                last = got.at[arrived, part, :]
                pltpu.make_async_copy(last, last, bwd_got.at[k + g]).wait()
            own = pl.ds(pl.multiple_of(g * GROUP, GROUP), GROUP)
            fs = [filters[i, own, :] for i in range(7)]

            def load(t):
                both = got[t, part, :].astype(f32)
                return both[:GROUP], both[GROUP:]

            both_signs = jnp.concatenate([fs[6], fs[6]], axis=0)
            if k == 0:
                got[0, part, :] = (got[1, part, :].astype(f32) * both_signs).astype(bf16)
            if k == chunks - 1:
                got[rows_all + 1, part, :] = (got[rows_all, part, :].astype(f32) * both_signs).astype(bf16)

            def some_rows(n, held):
                for u in range(GROUP):
                    t = n * GROUP + u
                    three = (*held, load(low + t + 2))
                    real = imag = 0.0
                    for i, (x, y) in enumerate(three):
                        real = real + fs[2 * i] * x - fs[2 * i + 1] * y
                        imag = imag + fs[2 * i] * y + fs[2 * i + 1] * x
                    mix[pl.ds(t, GROUP, stride=most), :] = real
                    mix[pl.ds(GROUP * most + t, GROUP, stride=most), :] = imag
                    held = three[1:]
                return held

            lax.fori_loop(0, (high - low) // GROUP, some_rows, (load(low), load(low + 1)))
            for i in range(GROUP):
                parts = [mix[pl.ds((r * GROUP + i) * most, high - low), :] for r in range(2)]
                both = jnp.concatenate(parts, axis=1).astype(bf16)
                field[g * GROUP + i, low:high, :] = jnp.dot(
                    both, perm[...], preferred_element_type=f32).astype(bf16)
            if k == chunks - 1:
                for i in range(GROUP):
                    s = g * GROUP + i
                    out = lax.dot_general(
                        field[s], table[s], (((0,), (0,)), ((), ())), preferred_element_type=f32)
                    out_ref[s] = out.astype(bf16).reshape(out_ref.shape[1:])
            return 0

        lax.fori_loop(0, groups, group, 0)
    for ref, sem in ((coeff, fwd_sent), (coeff, bwd_sent)):
        away = ref.at[:, pl.ds(0, count - 1)]
        pltpu.make_async_copy(away, away, sem).wait()


def on_device_rows(spec_in, legendre, mode_slot, w_in, b_in, w_out, kernel):
    lats, chans = lax.axis_size("lat"), lax.axis_size("chan")
    count = lats * chans
    slots, rows_all, degrees = legendre.shape
    width = spec_in.shape[2]
    own_rows = rows_all // count
    chunks = next(k for k in (4, 3, 2, 1) if own_rows % k == 0 and rows_all // k % 16 == 0)
    rows, span = own_rows // chunks, rows_all // chunks
    columns, groups, depth = NLON, slots // GROUP, 2 * slots
    hbm, vmem = pl.BlockSpec(memory_space=pl.ANY), pl.BlockSpec(memory_space=pltpu.VMEM)
    smem = pl.BlockSpec(memory_space=pltpu.SMEM)
    lag = 16 if chunks > 1 else 0
    bf16, f32 = jnp.bfloat16, jnp.float32
    out = pl.pallas_call(
        functools.partial(rows_kernel, lats, chans, chunks, columns),
        out_shape=pltpu.VMEM((slots, width, 2, degrees), bf16),
        in_specs=[smem] + [hbm] * 2 + [vmem] * 4,
        out_specs=vmem,
        scratch_shapes=[
            pltpu.VMEM((2, GROUP, span, degrees), f32),
            pltpu.VMEM((slots, width, 2, degrees), bf16),
            pltpu.VMEM((slots, rows_all, degrees), bf16),
            pltpu.VMEM((span * 2 * GROUP, width), f32),
            pltpu.VMEM((chunks, count, rows, depth, width), bf16),
            pltpu.VMEM((chunks, rows, chans, lats * depth, width), bf16),
            pltpu.VMEM((chunks, rows, chans, lats * depth, width), bf16),
            pltpu.VMEM((rows_all + 2, depth, width), bf16),
            pltpu.VMEM(((span + lag) * 2 * GROUP, width), f32),
            pltpu.VMEM((slots, rows_all, 2 * width), bf16),
            pltpu.VMEM((lats * depth, columns), bf16),
            pltpu.VMEM((columns, lats * depth), bf16),
            pltpu.VMEM((7, slots, width), f32),
            pltpu.VMEM((2 * width, 2 * width), bf16),
            pltpu.VMEM((2 * width, 2 * width), bf16),
            pltpu.VMEM((lats * depth, width), f32),
            pltpu.SemaphoreType.DMA((2,)),
            pltpu.SemaphoreType.DMA((groups,)),
            pltpu.SemaphoreType.DMA,
            pltpu.SemaphoreType.DMA((chunks,)),
            pltpu.SemaphoreType.DMA,
            pltpu.SemaphoreType.DMA((chunks + groups - 1,)),
        ],
        compiler_params=pltpu.CompilerParams(vmem_limit_bytes=52 * 1024 * 1024, has_side_effects=True, collective_id=0),
        name="rows",
    )(mode_slot, spec_in[:, 0], legendre, kernel.T, w_in, b_in[None, :], w_out)
    return out[:, None]


def solution(mesh):
    in_specs = (
        P("lat", None, "chan", None, None),
        P("lat", None, None),
        P(),
        P(),
        P(),
        P(),
        P("chan", None),
    )
    out_specs = P("lat", None, "chan", None, None)
    count = mesh.shape["lat"] * mesh.shape["chan"]

    def call(spec_in, legendre, *rest):
        samples, rows_all = spec_in.shape[1], legendre.shape[1]
        slots = spec_in.shape[0] // mesh.shape["lat"]
        by_rows = samples == 1 and rows_all % count == 0 and slots % GROUP == 0
        body = on_device_rows if by_rows else on_device
        return jax.shard_map(
            body, mesh=mesh, in_specs=in_specs, out_specs=out_specs, check_vma=False
        )(spec_in, legendre, *rest)

    return call
```

```python
import functools
import math

import jax
import jax.numpy as jnp
from jax import lax
from jax.experimental import pallas as pl
from jax.experimental.pallas import tpu as pltpu
from jax.sharding import PartitionSpec as P

NLON = 768


def with_halo(array, sides, width):
    for axis, dim in sides:
        count, length = (lax.axis_size(axis), array.shape[dim])
        up = [(i, (i + 1) % count) for i in range(count - 1)]
        down = [(j, i) for i, j in up]
        last = lax.slice_in_dim(array, length - width, length, axis=dim)
        first = lax.slice_in_dim(array, 0, width, axis=dim)
        before = lax.ppermute(last, axis, up)
        after = lax.ppermute(first, axis, down)
        array = jnp.concatenate([before, array, after], axis=dim)
    return array


def wave_table(modes, count):
    columns = jnp.arange(count, dtype=jnp.int32)
    phase = modes[:, None] * columns[None, :] % count
    angle = phase.astype(jnp.float32) * (2.0 * math.pi / count)
    factor = count ** (-0.5)
    return jnp.stack([jnp.cos(angle) * factor, -jnp.sin(angle) * factor], axis=1)


def on_device(spec_in, legendre, mode_slot, w_in, b_in, w_out, kernel):
    high = lax.Precision.HIGHEST
    slots_here = legendre.shape[0]
    lat_index = lax.axis_index("lat")
    local_modes = lax.dynamic_slice_in_dim(mode_slot, lat_index * slots_here, slots_here)
    degrees = jnp.arange(legendre.shape[2], dtype=jnp.int32)
    masked = jnp.where(
        degrees[None, None, :] >= local_modes[:, None, None], legendre, jnp.float32(0.0)
    )
    waves = wave_table(mode_slot, NLON)
    coeff = jnp.einsum("sbcrl,stl->sbcrt", spec_in.astype(jnp.float32), masked, precision=high)
    grid = jnp.einsum(
        "sbcrt,srp->btcp",
        lax.all_to_all(coeff, "lat", split_axis=4, concat_axis=0, tiled=True),
        waves,
        precision=high,
    ).astype(jnp.bfloat16)
    batch, rows_here, chan_here, columns = grid.shape
    whole = lax.all_gather(grid, "chan", axis=2, tiled=True)
    chan_index = lax.axis_index("chan")
    w_local = lax.dynamic_slice_in_dim(w_out, chan_index * chan_here, chan_here, 0)
    pre = jnp.einsum("hc,btcp->bthp", w_in, whole, preferred_element_type=jnp.float32)
    hidden = jax.nn.gelu(pre + b_in[None, None, :, None], approximate=True).astype(jnp.bfloat16)
    branch = jnp.einsum("ch,bthp->btcp", w_local, hidden, preferred_element_type=jnp.float32)
    mixed = (grid.astype(jnp.float32) + branch).astype(jnp.bfloat16)
    half = columns // 2
    last_row = lax.axis_size("lat") - 1
    padded = with_halo(mixed, (("lat", 1),), 1)
    upper = jnp.where(lat_index == 0, jnp.roll(mixed[:, 0:1], half, axis=3), padded[:, 0:1])
    lower = jnp.where(lat_index == last_row, jnp.roll(mixed[:, -1:], half, axis=3), padded[:, -1:])
    stacked = jnp.concatenate([upper, padded[:, 1:-1], lower], axis=1).astype(jnp.float32)
    wide = mixed.astype(jnp.float32)
    conv = jnp.zeros_like(wide)
    for i in range(3):
        band = stacked[:, i : i + rows_here]
        for j in range(3):
            conv = conv + kernel[:, 3 * i + j][None, None, :, None] * jnp.roll(band, 1 - j, axis=3)
    field = wide + conv
    modes = jnp.einsum("btcp,srp->sbcrt", field, waves, precision=high)
    return jnp.einsum(
        "sbcrt,stl->sbcrl",
        lax.all_to_all(modes, "lat", split_axis=0, concat_axis=4, tiled=True),
        masked,
        precision=high,
    ).astype(jnp.bfloat16)


GROUP = 8
LANES = 128


def cosine(phase, count):
    phase = phase - jnp.floor((phase + 0.5) * (1.0 / count)) * count
    turn = jnp.abs(phase - 0.5 * count) - 0.25 * count
    x = turn * (2.0 * math.pi / count)
    y = x * x
    total = jnp.full_like(y, -1.0 / math.factorial(11))
    for power, sign in ((9, 1.0), (7, -1.0), (5, 1.0), (3, -1.0), (1, 1.0)):
        total = total * y + sign / math.factorial(power)
    return total * x


def rows_kernel(lats, chans, chunks, columns, mode_ref, spec_ref, legendre_ref, taps_ref,
                w_in_ref, b_in_ref, w_out_ref, out_ref,
                raw, spec, table, stage, coeff, recv, send, got, mix, field, waves, waves_t, filters, perm, perm_t, marks, early,
                raw_got, spec_got, fwd_sent, fwd_got, bwd_sent, bwd_got):
    span, degrees = raw.shape[2:]
    slots = table.shape[0]
    count = lats * chans
    rows, rows_all = span // count, span * chunks
    depth, width = coeff.shape[3:]
    groups = slots // GROUP
    pair = 2 * GROUP
    lat, chan = lax.axis_index("lat"), lax.axis_index("chan")
    me = lat * chans + chan
    bf16, f32 = jnp.bfloat16, jnp.float32
    across = (((1,), (1,)), ((), ()))

    def fetch(n):
        return pltpu.make_async_copy(
            legendre_ref.at[pl.ds(n % groups * GROUP, GROUP), pl.ds(n // groups * span, span), :],
            raw.at[n % 2], raw_got.at[n % 2])

    def fetch_spec(g):
        part = pl.ds(g * GROUP, GROUP)
        return pltpu.make_async_copy(spec_ref.at[part], spec.at[part], spec_got.at[g])

    def to_all(block, landing, here, send_sem, recv_sem):
        def to_peer(i, _):
            to = (me + i) % count
            pltpu.make_async_remote_copy(
                src_ref=block(to), dst_ref=landing, send_sem=send_sem, recv_sem=recv_sem,
                device_id=(to // chans, to % chans), device_id_type=pl.DeviceIdType.MESH,
            ).start()
            return 0

        pltpu.make_async_copy(block(me), here, recv_sem).start()
        lax.fori_loop(1, count, to_peer, 0)

    barrier = pltpu.get_barrier_semaphore()

    def greet(i, _):
        to = (me + i) % count
        pl.semaphore_signal(
            barrier, inc=1, device_id=(to // chans, to % chans), device_id_type=pl.DeviceIdType.MESH)
        return 0

    lax.fori_loop(1, count, greet, 0)
    fetch(0).start()
    for g in range(groups):
        fetch_spec(g).start()
    i = lax.broadcasted_iota(jnp.int32, perm.shape, 0)
    j = lax.broadcasted_iota(jnp.int32, perm.shape, 1)
    perm[...] = jnp.where(j == i % width * 2 + i // width, 1.0, 0.0).astype(bf16)
    perm_t[...] = jnp.where(i == j % width * 2 + j // width, 1.0, 0.0).astype(bf16)
    lane = lax.broadcasted_iota(jnp.int32, (span, degrees), 1)

    def work_out(n):
        k, g = n // groups, n % groups
        fetch(n).wait()

        @pl.when(n < chunks * groups - 1)
        def _():
            fetch(n + 1).start()

        @pl.when(k == 0)
        def _():
            fetch_spec(g).wait()

        for i in range(GROUP):
            s = g * GROUP + i
            least = mode_ref[lat * slots + s]
            block = jnp.where(lane >= least, raw[n % 2, i], 0.0).astype(bf16)
            table[s, pl.ds(pl.multiple_of(k * span, span), span), :] = block
            value = lax.dot_general(
                block, spec[s].reshape(2 * width, degrees), across, preferred_element_type=f32)
            value = jnp.dot(value.astype(bf16), perm_t[...], preferred_element_type=f32)
            for r in range(2):
                stage[pl.ds(r * GROUP + i, span, stride=pair), :] = value[:, r * width : (r + 1) * width]
        part = pl.ds(pl.multiple_of(g * pair, pair), pair)
        coeff[k, :, :, part, :] = stage[...].astype(bf16).reshape(count, rows, pair, width)

    def send_group(g):
        part = pl.ds(g * pair, pair)
        landing = recv.at[0, :, chan, pl.ds(lat * depth + g * pair, pair), :]
        to_all(lambda to: coeff.at[0, to, :, part, :], landing, landing, fwd_sent, fwd_got.at[0])

    work_out(0)
    pl.semaphore_wait(barrier, count - 1)
    send_group(0)

    def forward(n, _):
        k, g = n // groups, n % groups
        work_out(n)

        @pl.when(k == 0)
        def _():
            send_group(g)

        @pl.when((k > 0) & (g == groups - 1))
        def _():
            landing = recv.at[k, :, chan, pl.ds(lat * depth, depth), :]
            to_all(lambda to: coeff.at[k, to], landing, landing, fwd_sent, fwd_got.at[k])

        return 0

    lax.fori_loop(1, chunks * groups, forward, 0)

    factor = columns ** -0.5
    size = lats * depth

    def mark(n, _):
        row = jnp.full((1, width), mode_ref[n], jnp.int32).astype(f32)
        for r in range(2):
            marks[pl.ds(n // GROUP * pair + r * GROUP + n % GROUP, 1), :] = row
        return 0

    lax.fori_loop(0, lats * slots, mark, 0)
    def wave_rows(n, _):
        here = pl.ds(pl.multiple_of(n * LANES, LANES), LANES)
        k = lax.broadcasted_iota(jnp.int32, (LANES, columns), 0) + n * LANES
        p = lax.broadcasted_iota(jnp.int32, (LANES, columns), 1)
        quarter = (k // GROUP) % 2 * (columns // 4)
        phase = marks[here, :1] * p.astype(f32) + quarter.astype(f32)
        waves[here, :] = (cosine(phase, columns) * factor).astype(bf16)
        return 0

    lax.fori_loop(0, size // LANES, wave_rows, 0)

    line = jnp.concatenate(
        [jnp.transpose(marks[n * LANES : (n + 1) * LANES, :LANES])[:1] for n in range(size // LANES)], axis=1)

    def wave_columns(n, _):
        here = pl.ds(pl.multiple_of(n * LANES, LANES), LANES)
        p = lax.broadcasted_iota(jnp.int32, (LANES, size), 0) + n * LANES
        k = lax.broadcasted_iota(jnp.int32, (LANES, size), 1)
        quarter = (k // GROUP) % 2 * (columns // 4)
        phase = line * p.astype(f32) + quarter.astype(f32)
        waves_t[here, :] = (cosine(phase, columns) * factor).astype(bf16)
        return 0

    lax.fori_loop(0, columns // LANES, wave_columns, 0)

    angle = jnp.concatenate(
        [marks[pl.ds(lat * depth + g * pair, GROUP), :] for g in range(groups)], axis=0)
    cos, minus_sin = cosine(angle, columns), cosine(angle + 0.25 * columns, columns)
    for i in range(3):
        left, here, right = (taps_ref[3 * i + j : 3 * i + j + 1, :] for j in range(3))
        filters[2 * i] = here + (left + right) * cos + (1.0 if i == 1 else 0.0)
        filters[2 * i + 1] = (left - right) * minus_sin
    filters[6] = cosine(angle * (columns // 2), columns)

    def one_chunk(k, _):
        pltpu.make_async_copy(recv.at[k], recv.at[k], fwd_got.at[k]).wait()

        def one_row(j, _):
            merged = jnp.concatenate([recv[k, j, i] for i in range(chans)], axis=1)
            grid = jnp.dot(waves_t[...], merged, preferred_element_type=f32).astype(bf16)
            pre = lax.dot_general(grid, w_in_ref[...], across, preferred_element_type=f32) + b_in_ref[...]
            hidden = jax.nn.gelu(pre, approximate=True).astype(bf16)
            branch = lax.dot_general(hidden, w_out_ref[...], across, preferred_element_type=f32)
            mixed = (grid.astype(f32) + branch).astype(bf16)
            modes = jnp.dot(waves[...], mixed, preferred_element_type=f32).astype(bf16)
            for i in range(chans):
                send[k, j, i] = modes[:, i * width : (i + 1) * width]
            return 0

        lax.fori_loop(0, rows, one_row, 0)
        landing = pl.ds(1 + k * span + me * rows, rows)

        @pl.when(k < chunks - 1)
        def _():
            here = got.at[landing]
            to_all(
                lambda to: send.at[k, :, to % chans, pl.ds((to // chans) * depth, depth), :],
                here, here, bwd_sent, bwd_got.at[k])

        @pl.when(k == chunks - 1)
        def _():
            def group(g, _):
                here = got.at[landing, pl.ds(g * pair, pair), :]
                to_all(
                    lambda to: send.at[k, :, to % chans, pl.ds((to // chans) * depth + g * pair, pair), :],
                    here, here, bwd_sent, bwd_got.at[k + g])
                return 0

            lax.fori_loop(0, groups, group, 0)

        return 0

    lax.fori_loop(0, chunks, one_chunk, 0)

    most = mix.shape[0] // pair
    lag = most - span

    for k in range(chunks):
        arrived = pl.ds(1 + k * span, span)
        if k < chunks - 1:
            pltpu.make_async_copy(got.at[arrived], got.at[arrived], bwd_got.at[k]).wait()
        low = max(k * span - lag, 0)
        high = rows_all if k == chunks - 1 else (k + 1) * span - lag

        def group(g, _):
            part = pl.ds(pl.multiple_of(g * pair, pair), pair)
            if k == chunks - 1:
                for i in range(GROUP if low else 0):
                    s = g * GROUP + i
                    early[i] = lax.dot_general(
                        field[s, :low], table[s, :low], (((0,), (0,)), ((), ())), preferred_element_type=f32)
                last = got.at[arrived, part, :]
                pltpu.make_async_copy(last, last, bwd_got.at[k + g]).wait()
            own = pl.ds(pl.multiple_of(g * GROUP, GROUP), GROUP)
            fs = [filters[i, own, :] for i in range(7)]

            def load(t):
                both = got[t, part, :].astype(f32)
                return both[:GROUP], both[GROUP:]

            both_signs = jnp.concatenate([fs[6], fs[6]], axis=0)
            if k == 0:
                got[0, part, :] = (got[1, part, :].astype(f32) * both_signs).astype(bf16)
            if k == chunks - 1:
                got[rows_all + 1, part, :] = (got[rows_all, part, :].astype(f32) * both_signs).astype(bf16)

            def some_rows(n, held):
                for u in range(GROUP):
                    t = n * GROUP + u
                    three = (*held, load(low + t + 2))
                    real = imag = 0.0
                    for i, (x, y) in enumerate(three):
                        real = real + fs[2 * i] * x - fs[2 * i + 1] * y
                        imag = imag + fs[2 * i] * y + fs[2 * i + 1] * x
                    mix[pl.ds(t, GROUP, stride=most), :] = real
                    mix[pl.ds(GROUP * most + t, GROUP, stride=most), :] = imag
                    held = three[1:]
                return held

            lax.fori_loop(0, (high - low) // GROUP, some_rows, (load(low), load(low + 1)))
            for i in range(GROUP):
                parts = [mix[pl.ds((r * GROUP + i) * most, high - low), :] for r in range(2)]
                both = jnp.concatenate(parts, axis=1).astype(bf16)
                field[g * GROUP + i, low:high, :] = jnp.dot(
                    both, perm[...], preferred_element_type=f32).astype(bf16)
            if k == chunks - 1:
                for i in range(GROUP):
                    s = g * GROUP + i
                    out = lax.dot_general(
                        field[s, low:], table[s, low:], (((0,), (0,)), ((), ())), preferred_element_type=f32)
                    if low:
                        out = out + early[i]
                    out_ref[s] = out.astype(bf16).reshape(out_ref.shape[1:])
            return 0

        lax.fori_loop(0, groups, group, 0)
    for ref, sem in ((coeff, fwd_sent), (coeff, bwd_sent)):
        away = ref.at[:, pl.ds(0, count - 1)]
        pltpu.make_async_copy(away, away, sem).wait()


def on_device_rows(spec_in, legendre, mode_slot, w_in, b_in, w_out, kernel):
    lats, chans = lax.axis_size("lat"), lax.axis_size("chan")
    count = lats * chans
    slots, rows_all, degrees = legendre.shape
    width = spec_in.shape[2]
    own_rows = rows_all // count
    chunks = next(k for k in (4, 3, 2, 1) if own_rows % k == 0 and rows_all // k % 16 == 0)
    rows, span = own_rows // chunks, rows_all // chunks
    columns, groups, depth = NLON, slots // GROUP, 2 * slots
    hbm, vmem = pl.BlockSpec(memory_space=pl.ANY), pl.BlockSpec(memory_space=pltpu.VMEM)
    smem = pl.BlockSpec(memory_space=pltpu.SMEM)
    lag = 16 if chunks > 1 else 0
    bf16, f32 = jnp.bfloat16, jnp.float32
    out = pl.pallas_call(
        functools.partial(rows_kernel, lats, chans, chunks, columns),
        out_shape=pltpu.VMEM((slots, width, 2, degrees), bf16),
        in_specs=[smem] + [hbm] * 2 + [vmem] * 4,
        out_specs=vmem,
        scratch_shapes=[
            pltpu.VMEM((2, GROUP, span, degrees), f32),
            pltpu.VMEM((slots, width, 2, degrees), bf16),
            pltpu.VMEM((slots, rows_all, degrees), bf16),
            pltpu.VMEM((span * 2 * GROUP, width), f32),
            pltpu.VMEM((chunks, count, rows, depth, width), bf16),
            pltpu.VMEM((chunks, rows, chans, lats * depth, width), bf16),
            pltpu.VMEM((chunks, rows, chans, lats * depth, width), bf16),
            pltpu.VMEM((rows_all + 2, depth, width), bf16),
            pltpu.VMEM(((span + lag) * 2 * GROUP, width), f32),
            pltpu.VMEM((slots, rows_all, 2 * width), bf16),
            pltpu.VMEM((lats * depth, columns), bf16),
            pltpu.VMEM((columns, lats * depth), bf16),
            pltpu.VMEM((7, slots, width), f32),
            pltpu.VMEM((2 * width, 2 * width), bf16),
            pltpu.VMEM((2 * width, 2 * width), bf16),
            pltpu.VMEM((lats * depth, width), f32),
            pltpu.VMEM((GROUP, 2 * width, degrees), f32),
            pltpu.SemaphoreType.DMA((2,)),
            pltpu.SemaphoreType.DMA((groups,)),
            pltpu.SemaphoreType.DMA,
            pltpu.SemaphoreType.DMA((chunks,)),
            pltpu.SemaphoreType.DMA,
            pltpu.SemaphoreType.DMA((chunks + groups - 1,)),
        ],
        compiler_params=pltpu.CompilerParams(vmem_limit_bytes=54 * 1024 * 1024, has_side_effects=True, collective_id=0),
        name="rows",
    )(mode_slot, spec_in[:, 0], legendre, kernel.T, w_in, b_in[None, :], w_out)
    return out[:, None]


def solution(mesh):
    in_specs = (
        P("lat", None, "chan", None, None),
        P("lat", None, None),
        P(),
        P(),
        P(),
        P(),
        P("chan", None),
    )
    out_specs = P("lat", None, "chan", None, None)
    count = mesh.shape["lat"] * mesh.shape["chan"]

    def call(spec_in, legendre, *rest):
        samples, rows_all = spec_in.shape[1], legendre.shape[1]
        slots = spec_in.shape[0] // mesh.shape["lat"]
        by_rows = samples == 1 and rows_all % count == 0 and slots % GROUP == 0
        body = on_device_rows if by_rows else on_device
        return jax.shard_map(
            body, mesh=mesh, in_specs=in_specs, out_specs=out_specs, check_vma=False
        )(spec_in, legendre, *rest)

    return call
```
